128 devices in a mesh: dp: 1, sp: 128 (over z, y, x, core).
Axes of the slice: x: 4, y: 4, z: 4, core: 2. Of those that a mesh axis runs over, the one named last changes fastest.
Arguments:
- x_one: bfloat16 [2048, 7168], P(('dp', 'sp'))
- seg_one: int32 [2048], P(('dp', 'sp'))
- pos_one: int32 [2048], P(('dp', 'sp'))
- x_two: bfloat16 [2048, 7168], P(('dp', 'sp'))
- seg_two: int32 [2048], P(('dp', 'sp'))
- pos_two: int32 [2048], P(('dp', 'sp'))
- w_qdown: bfloat16 [7168, 1536], replicated
- gain_q: bfloat16 [1536], replicated
- w_qup: bfloat16 [1536, 24576], replicated
- w_kvdown: bfloat16 [7168, 576], replicated
- gain_kv: bfloat16 [512], replicated
- w_kvup: bfloat16 [512, 32768], replicated
- w_out: bfloat16 [16384, 7168], replicated
Outputs:
- output 1: bfloat16 [2048, 7168], P(('dp', 'sp'))
- output 2: bfloat16 [2048, 7168], P(('dp', 'sp'))
All inputs are finite; a program needn't handle non-finite values.
Results may differ from the reference program's by a relative error of at most 0.0140363.
Values are sent between devices in bfloat16 or wider.
A program may use at most 1.5 GiB of HBM per device.

```python
import jax
import jax.numpy as jnp
from jax import lax

TOKENS = 2048
D_MODEL = 7168
HEADS = 128
Q_LAT = 1536
KV_LAT = 512
ROPE_DIM = 64
NOPE_DIM = 128
V_DIM = 128
PROMPTS = 2
QK_DIM = NOPE_DIM + ROPE_DIM
KV_DOWN = KV_LAT + ROPE_DIM
ROPE_BASE = 10000.0
NORM_EPS = 1e-6


def draw_layout(draw_key):
    shuffled = jax.random.permutation(draw_key, TOKENS - 1) + 1
    cut_points = jnp.sort(shuffled[:PROMPTS - 1]).astype(jnp.int32)
    tok_index = jnp.arange(TOKENS, dtype=jnp.int32)
    prompt_ids = jnp.searchsorted(cut_points, tok_index, side='right').astype(jnp.int32)
    prompt_start = jnp.concatenate([jnp.zeros((1,), jnp.int32), cut_points])
    return prompt_ids, tok_index - prompt_start[prompt_ids]


def normal_weight(draw_key, arr_shape, fan_in, scale_by):
    return (jax.random.normal(draw_key, arr_shape, jnp.float32) * scale_by * fan_in ** -0.5).astype(jnp.bfloat16)


def setup_inputs(seed: int = 0, part: int = 0) -> dict:
    part_keys = jax.random.split(jax.random.fold_in(jax.random.key(seed), part), 4)
    weight_keys = jax.random.split(jax.random.key(seed + 1), 7)
    seg_one, pos_one = draw_layout(part_keys[0])
    seg_two, pos_two = draw_layout(part_keys[1])
    return {
        'x_one': jax.random.normal(part_keys[2], (TOKENS, D_MODEL), jnp.float32).astype(jnp.bfloat16),
        'seg_one': seg_one,
        'pos_one': pos_one,
        'x_two': jax.random.normal(part_keys[3], (TOKENS, D_MODEL), jnp.float32).astype(jnp.bfloat16),
        'seg_two': seg_two,
        'pos_two': pos_two,
        'w_qdown': normal_weight(weight_keys[0], (D_MODEL, Q_LAT), D_MODEL, 1.0),
        'gain_q': jax.random.uniform(weight_keys[1], (Q_LAT,), jnp.float32, 0.5, 1.5).astype(jnp.bfloat16),
        'w_qup': normal_weight(weight_keys[2], (Q_LAT, HEADS * QK_DIM), Q_LAT, 1.0),
        'w_kvdown': normal_weight(weight_keys[3], (D_MODEL, KV_DOWN), D_MODEL, 1.0),
        'gain_kv': jax.random.uniform(weight_keys[4], (KV_LAT,), jnp.float32, 0.5, 1.5).astype(jnp.bfloat16),
        'w_kvup': normal_weight(weight_keys[5], (KV_LAT, HEADS * (NOPE_DIM + V_DIM)), KV_LAT, 1.0),
        'w_out': normal_weight(weight_keys[6], (HEADS * V_DIM, D_MODEL), HEADS * V_DIM, 2.0),
    }


def rms_scale(pre_norm, gain_vec):
    mean_sq = jnp.mean(pre_norm * pre_norm, axis=-1, keepdims=True)
    return (pre_norm * lax.rsqrt(mean_sq + NORM_EPS) * gain_vec.astype(jnp.float32)).astype(jnp.bfloat16)


def rope_tables(positions):
    half_dim = ROPE_DIM // 2
    inv_freq = ROPE_BASE ** (-jnp.arange(half_dim, dtype=jnp.float32) / half_dim)
    angles = positions.astype(jnp.float32)[..., None] * inv_freq
    return jnp.cos(angles), jnp.sin(angles)


def rope_rotate(rot_in, cos_tab, sin_tab):
    half_dim = ROPE_DIM // 2
    first_half = rot_in[..., :half_dim]
    second_half = rot_in[..., half_dim:]
    return jnp.concatenate([first_half * cos_tab - second_half * sin_tab, second_half * cos_tab + first_half * sin_tab], axis=-1)


def mla_block(tokens_in, prompt_ids, positions, w_qdown, gain_q, w_qup, w_kvdown, gain_kv, w_kvup, w_out):
    q_latent = rms_scale(jnp.dot(tokens_in, w_qdown, preferred_element_type=jnp.float32), gain_q)
    kv_raw = jnp.dot(tokens_in, w_kvdown, preferred_element_type=jnp.float32)
    kv_latent = rms_scale(kv_raw[:, :KV_LAT], gain_kv)
    cos_tab, sin_tab = rope_tables(positions)
    k_rope = rope_rotate(kv_raw[:, KV_LAT:], cos_tab, sin_tab).astype(jnp.bfloat16)
    allowed = (prompt_ids[:, None] == prompt_ids[None, :]) & (positions[None, :] <= positions[:, None])
    wq_heads = w_qup.reshape(Q_LAT, HEADS, QK_DIM).transpose(1, 0, 2)
    wkv_heads = w_kvup.reshape(KV_LAT, HEADS, NOPE_DIM + V_DIM).transpose(1, 0, 2)

    def one_head(head_weights):
        wq_head, wkv_head = head_weights
        q_head = jnp.dot(q_latent, wq_head, preferred_element_type=jnp.float32)
        q_nope = q_head[:, :NOPE_DIM].astype(jnp.bfloat16)
        q_rope = rope_rotate(q_head[:, NOPE_DIM:], cos_tab, sin_tab).astype(jnp.bfloat16)
        kv_head = jnp.dot(kv_latent, wkv_head, preferred_element_type=jnp.float32).astype(jnp.bfloat16)
        q_cat = jnp.concatenate([q_nope, q_rope], axis=1)
        k_cat = jnp.concatenate([kv_head[:, :NOPE_DIM], k_rope], axis=1)
        scores = jnp.dot(q_cat, k_cat.T, preferred_element_type=jnp.float32) * QK_DIM ** -0.5
        attn_prob = jax.nn.softmax(jnp.where(allowed, scores, -1e30), axis=-1).astype(jnp.bfloat16)
        return jnp.dot(attn_prob, kv_head[:, NOPE_DIM:], preferred_element_type=jnp.float32).astype(jnp.bfloat16)

    head_out = lax.map(one_head, (wq_heads, wkv_heads))
    attn_flat = head_out.transpose(1, 0, 2).reshape(TOKENS, HEADS * V_DIM)
    return jnp.dot(attn_flat, w_out, preferred_element_type=jnp.float32).astype(jnp.bfloat16)


def reference(x_one, seg_one, pos_one, x_two, seg_two, pos_two, w_qdown, gain_q, w_qup, w_kvdown, gain_kv, w_kvup, w_out):
    y_one = mla_block(x_one, seg_one, pos_one, w_qdown, gain_q, w_qup, w_kvdown, gain_kv, w_kvup, w_out)
    y_two = mla_block(x_two, seg_two, pos_two, w_qdown, gain_q, w_qup, w_kvdown, gain_kv, w_kvup, w_out)
    return (y_one, y_two)
```

```python
import functools

import jax
import jax.numpy as jnp
from jax import lax
from jax.experimental import pallas as pl
from jax.experimental.pallas import tpu as pltpu
from jax.sharding import PartitionSpec as P

D_MODEL = 7168
HEADS = 128
Q_LAT = 1536
KV_LAT = 512
ROPE_DIM = 64
NOPE_DIM = 128
V_DIM = 128
QK_DIM = NOPE_DIM + ROPE_DIM
ROPE_BASE = 10000.0
NORM_EPS = 1e-6

ROWS = 16
RING = 4
GROUP = 2 * RING
G_HEADS = HEADS // GROUP
TOKENS = 2048
KV_W = 2 * KV_LAT + 2 * ROPE_DIM
Q_W = KV_LAT + 2 * ROPE_DIM
MESH = pl.DeviceIdType.MESH

COLORS = (((0, 384), (2, 1, 0)), ((384, 768), (1, 0, 2)), ((768, 1152), (0, 2, 1)))


def coords():
    me = lax.axis_index("sp")
    return me // 32, lax.rem(me // 8, 4), lax.rem(me // 2, 4), lax.rem(me, 2)


def device(z, y, x, c):
    return {"sp": ((z * RING + y) * RING + x) * 2 + c}


def shifted(pos, axis, k):
    out = list(pos)
    out[axis] = lax.rem(pos[axis] + k, RING)
    return tuple(out)


def gather_kernel(kv_in, q_in, tab_in, kv_ref, q_ref, tab_ref, kv_send, kv_recv, q_send, q_recv, t_send, t_recv,
                  d_send, d_recv, dq_send, dq_recv):
    z, y, x, c = coords()
    pos = (z, y, x)
    other = device(z, y, x, 1 - c)

    barrier = pltpu.get_barrier_semaphore()
    for axis in range(3):
        for k in range(1, RING):
            pl.semaphore_signal(barrier, inc=1, device_id=device(*shifted(pos, axis, k), c), device_id_type=MESH)
    pl.semaphore_signal(barrier, inc=1, device_id=other, device_id_type=MESH)
    kv_ref[z, y, x, c] = kv_in[...]
    q_ref[:, z, c] = q_in[...]
    tab_ref[:, z, c] = tab_in[...]
    pl.semaphore_wait(barrier, 10)

    def kv_piece(color, phase, at):
        (lo, hi), order = COLORS[color]
        index = [at[0], at[1], at[2]]
        for axis in order[:phase]:
            index[axis] = slice(None)
        return kv_ref.at[index[0], index[1], index[2], c, :, pl.ds(lo, hi - lo)]

    def kv_copy(color, phase, k, at, to):
        piece = kv_piece(color, phase, at)
        return pltpu.make_async_remote_copy(
            src_ref=piece, dst_ref=piece, send_sem=kv_send.at[color, phase, k - 1],
            recv_sem=kv_recv.at[color, phase, k - 1], device_id=to, device_id_type=MESH)

    def pass_copy(color, k, at):
        piece = kv_piece(color, 2, at)
        return pltpu.make_async_remote_copy(
            src_ref=piece, dst_ref=piece, send_sem=d_send.at[color, k],
            recv_sem=d_recv.at[color, k], device_id=other, device_id_type=MESH)

    def other_piece(color, k, at):
        (lo, hi), order = COLORS[color]
        index = [slice(None)] * 3
        index[order[2]] = at[order[2]]
        piece = kv_ref.at[index[0], index[1], index[2], 1 - c, :, pl.ds(lo, hi - lo)]
        return pltpu.make_async_remote_copy(
            src_ref=piece, dst_ref=piece, send_sem=d_send.at[color, k],
            recv_sem=d_recv.at[color, k], device_id=other, device_id_type=MESH)

    def q_copy(k, zz, cc, to, send, recv):
        return pltpu.make_async_remote_copy(
            src_ref=q_ref.at[:, zz, cc], dst_ref=q_ref.at[:, zz, cc], send_sem=send, recv_sem=recv,
            device_id=to, device_id_type=MESH)

    def t_copy(k, zz, cc, to, send, recv):
        return pltpu.make_async_remote_copy(
            src_ref=tab_ref.at[:, zz, cc], dst_ref=tab_ref.at[:, zz, cc], send_sem=send, recv_sem=recv,
            device_id=to, device_id_type=MESH)

    for phase in range(3):
        for color in range(3):
            axis = COLORS[color][1][phase]
            for k in range(1, RING):
                kv_copy(color, phase, k, pos, device(*shifted(pos, axis, k), c)).start()
        if phase == 0:
            for k in range(1, RING):
                to = device(*shifted(pos, 0, k), c)
                t_copy(k, z, c, to, t_send.at[k - 1], t_recv.at[k - 1]).start()
                q_copy(k, z, c, to, q_send.at[k - 1], q_recv.at[k - 1]).start()
            t_copy(0, z, c, other, dq_send.at[0, 0], dq_recv.at[0, 0]).start()
            q_copy(0, z, c, other, dq_send.at[1, 0], dq_recv.at[1, 0]).start()
        if phase == 2:
            for color in range(3):
                pass_copy(color, 0, pos).start()
            for k in range(1, RING):
                zz = lax.rem(z + RING - k, RING)
                t_copy(k, zz, c, other, t_send.at[k - 1], t_recv.at[k - 1]).wait_recv()
                t_copy(k, zz, c, other, dq_send.at[0, k], dq_recv.at[0, k]).start()
                q_copy(k, zz, c, other, q_send.at[k - 1], q_recv.at[k - 1]).wait_recv()
                q_copy(k, zz, c, other, dq_send.at[1, k], dq_recv.at[1, k]).start()
        for k in (1, 3, 2):
            for color in range(3):
                axis = COLORS[color][1][phase]
                source = shifted(pos, axis, RING - k)
                kv_copy(color, phase, k, source, other).wait_recv()
                if phase == 2:
                    pass_copy(color, k, source).start()

    for k in range(RING):
        zz = lax.rem(z + RING - k, RING)
        t_copy(k, zz, 1 - c, other, dq_send.at[0, k], dq_recv.at[0, k]).wait()
        q_copy(k, zz, 1 - c, other, dq_send.at[1, k], dq_recv.at[1, k]).wait()
        for color in range(3):
            source = shifted(pos, COLORS[color][1][2], RING - k)
            other_piece(color, k, source).wait()
    for k in range(1, RING):
        t_copy(k, z, c, other, t_send.at[k - 1], t_recv.at[k - 1]).wait_send()
        q_copy(k, z, c, other, q_send.at[k - 1], q_recv.at[k - 1]).wait_send()
        for phase in range(3):
            for color in range(3):
                kv_copy(color, phase, k, pos, other).wait_send()


def gather(kv_loc, q_loc, tab_loc):
    dma = pltpu.SemaphoreType.DMA
    vmem = pl.BlockSpec(memory_space=pltpu.VMEM)
    return pl.pallas_call(
        gather_kernel,
        out_shape=(jax.ShapeDtypeStruct((RING, RING, RING, 2, ROWS, KV_W), jnp.bfloat16),
                   jax.ShapeDtypeStruct((2, RING, 2, ROWS, Q_LAT), jnp.bfloat16),
                   jax.ShapeDtypeStruct((2, RING, 2, ROWS, 128), jnp.float32)),
        in_specs=[vmem] * 3,
        out_specs=(vmem,) * 3,
        scratch_shapes=[dma((3, 3, 3)), dma((3, 3, 3)), dma((3,)), dma((3,)), dma((3,)), dma((3,)),
                        dma((3, 4)), dma((3, 4)), dma((2, 4)), dma((2, 4))],
        compiler_params=pltpu.CompilerParams(collective_id=0, has_side_effects=True),
        name="latent_gather",
    )(kv_loc, q_loc, tab_loc)


WQ_CHUNKS = 4


def attention_kernel(q_ref, tab_ref, kv_ref, wq_hbm, wkv_hbm, o_ref, wq, wkv, q_eff, o_lat, wq_sem, wkv_sem):
    z, y, x, c = coords()
    rank = z * 2 + c
    rows = 2 * RING * 2 * ROWS
    unit_rows = 2 * ROWS
    wcols = G_HEADS * QK_DIM // WQ_CHUNKS

    def wq_copy(i):
        return pltpu.make_async_copy(
            wq_hbm.at[:, pl.ds(pl.multiple_of(rank * (G_HEADS * QK_DIM) + i * wcols, 128), wcols)],
            wq.at[i], wq_sem.at[i])

    wkv_copy = pltpu.make_async_copy(
        wkv_hbm.at[:, pl.ds(pl.multiple_of(rank * (G_HEADS * 256), 128), G_HEADS * 256)], wkv, wkv_sem)
    wq_copy(0).start()
    wkv_copy.start()
    for i in range(1, WQ_CHUNKS):
        wq_copy(i).start()

    lane = lax.broadcasted_iota(jnp.int32, (rows, 128), 1)
    tab = tab_ref[...]
    cos_t = jnp.where(lane < 32, tab, jnp.where(lane < 64, pltpu.roll(tab, 32, 1), 0.0))
    sin_b = jnp.where((lane >= 32) & (lane < 64), tab, 0.0)
    sin_a = jnp.where(lane < 32, -pltpu.roll(tab, 96, 1), 0.0)

    def put_rope(head, part):
        out = part * cos_t + pltpu.roll(part, 32, 1) * sin_b + pltpu.roll(part, 96, 1) * sin_a
        half = rows // 2
        out = jnp.concatenate([out[:half], pltpu.roll(out[half:], 64, 1)], axis=0)
        q_eff[:, head, :, KV_LAT:] = out.astype(jnp.bfloat16).reshape(2 * RING, unit_rows, 128)

    def put_nope(head, part):
        w_k = wkv[:, pl.ds(pl.multiple_of(head * 256, 256), 128)]
        out = lax.dot_general(part.astype(jnp.bfloat16), w_k, (((1,), (1,)), ((), ())), preferred_element_type=jnp.float32)
        q_eff[:, head, :, :KV_LAT] = out.astype(jnp.bfloat16).reshape(2 * RING, unit_rows, KV_LAT)

    pairs = wcols // (2 * QK_DIM)
    for i in range(WQ_CHUNKS):
        wq_copy(i).wait()
        if i == 0:
            wkv_copy.wait()

        @pl.loop(0, pairs)
        def _(p):
            cols = pl.ds(pl.multiple_of(p * (2 * QK_DIM), 128), 2 * QK_DIM)
            f = jnp.dot(q_ref[...], wq[i, :, cols], preferred_element_type=jnp.float32)
            head = (i * pairs + p) * 2
            put_nope(head, f[:, :128])
            put_rope(head, f[:, 128:256])
            mid = pltpu.roll(f[:, 128:256], 64, 1)
            last = pltpu.roll(f[:, 256:384], 64, 1)
            put_nope(head + 1, jnp.where(lane < 64, mid, last))
            put_rope(head + 1, last)

    chunk_heads = 8
    scale2 = (QK_DIM ** -0.5) * 1.4426950408889634
    tok = lax.broadcasted_iota(jnp.int32, (unit_rows, 1), 0)
    for zz in range(RING):
        length = (zz + 1) * 512
        key = lax.broadcasted_iota(jnp.int32, (unit_rows, length), 1)
        q_tok = zz * 512 + y * 128 + x * 32 + tok

        for mb in range(2):
            unit = mb * RING + zz
            p0 = tab_ref[unit * unit_rows:(unit + 1) * unit_rows, 64:65].astype(jnp.int32)
            cap = jnp.where((key <= q_tok) & (key >= q_tok - p0), 3e38, -1e30).astype(jnp.float32)

            @pl.loop(0, G_HEADS // chunk_heads)
            def _(j):
                heads = pl.ds(j * chunk_heads, chunk_heads)
                q = q_eff[unit, heads].reshape(chunk_heads * unit_rows, Q_W)
                keys = kv_ref[:length, mb * KV_LAT:(mb + 1) * KV_LAT]
                trans = (((1,), (1,)), ((), ()))
                s = lax.dot_general(q[:, :KV_LAT], keys, trans, preferred_element_type=jnp.float32)
                s = s + lax.dot_general(q[:, KV_LAT:], kv_ref[:length, 2 * KV_LAT:], trans, preferred_element_type=jnp.float32)
                s = jnp.minimum(s.reshape(chunk_heads, unit_rows, length), cap[None])
                top = jnp.max(s, axis=-1, keepdims=True)
                e = jnp.exp2((s - top) * scale2)
                total = jnp.sum(e, axis=-1, keepdims=True)
                e = e.astype(jnp.bfloat16).reshape(chunk_heads * unit_rows, length)
                o = jnp.dot(e, keys, preferred_element_type=jnp.float32).reshape(chunk_heads, unit_rows, KV_LAT)
                o_lat[heads, unit * unit_rows:(unit + 1) * unit_rows, :] = (o / total).astype(jnp.bfloat16)

    @pl.loop(0, G_HEADS)
    def _(h):
        w_v = wkv[:, pl.ds(pl.multiple_of(h * 256 + 128, 128), 128)]
        o_ref[:, pl.ds(pl.multiple_of(h * 128, 128), 128)] = jnp.dot(
            o_lat[h], w_v, preferred_element_type=jnp.float32).astype(jnp.bfloat16)


def attention(q_all, tab_all, kv_all, w_qup, w_kvup):
    rows = 2 * RING * 2 * ROWS
    vmem = pl.BlockSpec(memory_space=pltpu.VMEM)
    hbm = pl.BlockSpec(memory_space=pl.ANY)
    return pl.pallas_call(
        attention_kernel,
        out_shape=jax.ShapeDtypeStruct((rows, G_HEADS * V_DIM), jnp.bfloat16),
        in_specs=[vmem, vmem, vmem, hbm, hbm],
        out_specs=vmem,
        scratch_shapes=[
            pltpu.VMEM((WQ_CHUNKS, Q_LAT, G_HEADS * QK_DIM // WQ_CHUNKS), jnp.bfloat16),
            pltpu.VMEM((KV_LAT, G_HEADS * 256), jnp.bfloat16),
            pltpu.VMEM((2 * RING, G_HEADS, 2 * ROWS, Q_W), jnp.bfloat16),
            pltpu.VMEM((G_HEADS, rows, KV_LAT), jnp.bfloat16),
            pltpu.SemaphoreType.DMA((WQ_CHUNKS,)),
            pltpu.SemaphoreType.DMA,
        ],
        compiler_params=pltpu.CompilerParams(vmem_limit_bytes=60 * 2 ** 20),
        name="latent_attention",
    )(q_all, tab_all, kv_all, w_qup, w_kvup)


W_ROWS = 1024
W_SLOTS = 5
HALF_N = D_MODEL // 2
OUT_ROWS = 4 * ROWS


def out_kernel(o_ref, w_hbm, y_one, y_two, o_all, w_buf, acc, y_send, w_sem, a_send, a_recv, d_send, d_recv, y_ssem, y_rsem):
    z, y, x, c = coords()
    pos = (z, y, x)
    other = device(z, y, x, 1 - c)
    k_cols = G_HEADS * V_DIM
    per_rank = k_cols // W_ROWS
    steps = GROUP * per_rank

    order = ((0, 0), (0, 1), (1, 0), (3, 0), (1, 1), (2, 0), (3, 1), (2, 1))

    def rank_at(j):
        rank = jnp.int32(0)
        for i, (k, flip) in enumerate(order):
            cc = c if flip == 0 else 1 - c
            rank = jnp.where(j == i, lax.rem(z + RING - k, RING) * 2 + cc, rank)
        return rank

    def w_copy(t):
        rank = rank_at(t // per_rank)
        row = pl.multiple_of(rank * k_cols + lax.rem(t, per_rank) * W_ROWS, W_ROWS)
        slot = lax.rem(t, W_SLOTS)
        return pltpu.make_async_copy(
            w_hbm.at[pl.ds(row, W_ROWS), pl.ds(pl.multiple_of(c * HALF_N, 128), HALF_N)], w_buf.at[slot], w_sem.at[slot])

    barrier = pltpu.get_barrier_semaphore()
    for k in range(1, RING):
        pl.semaphore_signal(barrier, inc=1, device_id=device(*shifted(pos, 0, k), c), device_id_type=MESH)
    pl.semaphore_signal(barrier, inc=1, device_id=other, device_id_type=MESH)
    for t in range(W_SLOTS - 1):
        w_copy(jnp.int32(t)).start()
    pl.semaphore_wait(barrier, 4)

    me = z * 2 + c

    def ring_copy(k, src_rank, src_z, to):
        return pltpu.make_async_remote_copy(
            src_ref=o_ref.at[:, src_z], dst_ref=o_all.at[src_rank], send_sem=a_send.at[k - 1],
            recv_sem=a_recv.at[k - 1], device_id=to, device_id_type=MESH)

    def pass_copy(k, rank, src):
        return pltpu.make_async_remote_copy(
            src_ref=src, dst_ref=o_all.at[rank], send_sem=d_send.at[k], recv_sem=d_recv.at[k],
            device_id=other, device_id_type=MESH)

    for k in (1, 3, 2):
        zz = lax.rem(z + k, RING)
        ring_copy(k, me, zz, device(zz, y, x, c)).start()
    pass_copy(0, me, o_ref.at[:, z]).start()
    o_all[me] = o_ref[:, z]
    acc[...] = jnp.zeros_like(acc)

    @pl.loop(0, steps)
    def _(t):
        @pl.when(t + W_SLOTS - 1 < steps)
        def _():
            w_copy(t + W_SLOTS - 1).start()

        for i, (k, flip) in enumerate(order):
            if i == 0:
                continue

            @pl.when(t == i * per_rank)
            def _(i=i, k=k, flip=flip):
                zz = lax.rem(z + RING - k, RING)
                if flip == 0:
                    ring_copy(k, zz * 2 + c, z, other).wait_recv()
                    pass_copy(k, zz * 2 + c, o_all.at[zz * 2 + c]).start()
                else:
                    pass_copy(k, zz * 2 + 1 - c, o_all.at[zz * 2 + 1 - c]).wait_recv()

        rank = rank_at(t // per_rank)
        w_copy(t).wait()
        lhs = o_all[rank, :, :, :, pl.ds(pl.multiple_of(lax.rem(t, per_rank) * W_ROWS, W_ROWS), W_ROWS)].reshape(OUT_ROWS, W_ROWS)
        slot = lax.rem(t, W_SLOTS)
        step_n = 512
        for n in range(HALF_N // step_n):
            cols = slice(n * step_n, (n + 1) * step_n)
            acc[:, cols] += jnp.dot(lhs, w_buf[slot, :, cols], preferred_element_type=jnp.float32)

    acc4 = acc.reshape(2, 2, ROWS, HALF_N)
    my_cols = pl.ds(pl.multiple_of(c * HALF_N, 128), HALF_N)
    for mb, y_ref in enumerate((y_one, y_two)):
        y_send[mb] = acc4[mb, 1 - c].astype(jnp.bfloat16)
    for mb, y_ref in enumerate((y_one, y_two)):
        y_ref[:, my_cols] = acc4[mb, c].astype(jnp.bfloat16)

    def y_copy(mb, y_ref, cols):
        return pltpu.make_async_remote_copy(
            src_ref=y_send.at[mb], dst_ref=y_ref.at[:, cols], send_sem=y_ssem.at[mb], recv_sem=y_rsem.at[mb],
            device_id=other, device_id_type=MESH)

    for mb, y_ref in enumerate((y_one, y_two)):
        y_copy(mb, y_ref, my_cols).start()
    their_cols = pl.ds(pl.multiple_of((1 - c) * HALF_N, 128), HALF_N)
    for mb, y_ref in enumerate((y_one, y_two)):
        y_copy(mb, y_ref, their_cols).wait()
    for k in range(1, RING):
        ring_copy(k, me, z, other).wait_send()
    for k in range(RING):
        pass_copy(k, me, o_all.at[me]).wait_send()


def project_out(o, w_out):
    dma = pltpu.SemaphoreType.DMA
    vmem = pl.BlockSpec(memory_space=pltpu.VMEM)
    hbm = pl.BlockSpec(memory_space=pl.ANY)
    y_shape = jax.ShapeDtypeStruct((ROWS, D_MODEL), jnp.bfloat16)
    return pl.pallas_call(
        out_kernel,
        out_shape=(y_shape, y_shape),
        in_specs=[vmem, hbm],
        out_specs=(vmem, vmem),
        scratch_shapes=[
            pltpu.VMEM((GROUP, 2, 2, ROWS, G_HEADS * V_DIM), jnp.bfloat16),
            pltpu.VMEM((W_SLOTS, W_ROWS, HALF_N), jnp.bfloat16),
            pltpu.VMEM((OUT_ROWS, HALF_N), jnp.float32),
            pltpu.VMEM((2, ROWS, HALF_N), jnp.bfloat16),
            dma((W_SLOTS,)), dma((3,)), dma((3,)), dma((4,)), dma((4,)), dma((2,)), dma((2,)),
        ],
        compiler_params=pltpu.CompilerParams(collective_id=1, has_side_effects=True, vmem_limit_bytes=60 * 2 ** 20),
        name="out_projection",
    )(o, w_out)


def rms_scale(pre_norm, gain_vec):
    mean_sq = jnp.mean(pre_norm * pre_norm, axis=-1, keepdims=True)
    return (pre_norm * lax.rsqrt(mean_sq + NORM_EPS) * gain_vec.astype(jnp.float32)).astype(jnp.bfloat16)


def latents(x_one, pos_one, x_two, pos_two, w_qdown, gain_q, w_kvdown, gain_kv):
    half_dim = ROPE_DIM // 2
    rows_x = jnp.concatenate([x_one, x_two], axis=0)
    pos = jnp.concatenate([pos_one, pos_two], axis=0).astype(jnp.float32)[:, None]
    q_latent = rms_scale(jnp.dot(rows_x, w_qdown, preferred_element_type=jnp.float32), gain_q)
    kv_raw = jnp.dot(rows_x, w_kvdown, preferred_element_type=jnp.float32)
    kv_latent = rms_scale(kv_raw[:, :KV_LAT], gain_kv)
    inv_freq = ROPE_BASE ** (-jnp.arange(half_dim, dtype=jnp.float32) / half_dim)
    angles = pos * inv_freq
    cos_tab, sin_tab = jnp.cos(angles), jnp.sin(angles)
    a, b = kv_raw[:, KV_LAT:KV_LAT + half_dim], kv_raw[:, KV_LAT + half_dim:]
    k_rope = jnp.concatenate([a * cos_tab - b * sin_tab, b * cos_tab + a * sin_tab], axis=-1).astype(jnp.bfloat16)
    kv_loc = jnp.concatenate([kv_latent[:ROWS], kv_latent[ROWS:], k_rope[:ROWS], k_rope[ROWS:]], axis=1)
    tab = jnp.concatenate([cos_tab, sin_tab, jnp.broadcast_to(pos, (2 * ROWS, ROPE_DIM))], axis=1)
    return kv_loc, q_latent.reshape(2, ROWS, Q_LAT), tab.reshape(2, ROWS, 128)


def solution(mesh):
    tok_spec = P(('dp', 'sp'), None)
    idx_spec = P(('dp', 'sp'))

    def local_body(x_one, seg_one, pos_one, x_two, seg_two, pos_two, w_qdown, gain_q, w_qup, w_kvdown, gain_kv, w_kvup, w_out):
        kv_loc, q_loc, tab_loc = latents(x_one, pos_one, x_two, pos_two, w_qdown, gain_q, w_kvdown, gain_kv)
        kv_all, q_all, tab_all = gather(kv_loc, q_loc, tab_loc)
        o = attention(q_all.reshape(-1, Q_LAT), tab_all.reshape(-1, 128), kv_all.reshape(TOKENS, KV_W), w_qup, w_kvup)
        return project_out(o.reshape(2, RING, 2, ROWS, -1), w_out)

    return jax.shard_map(local_body, mesh=mesh, in_specs=(tok_spec, idx_spec, idx_spec, tok_spec, idx_spec, idx_spec, P(), P(), P(), P(), P(), P(), P()), out_specs=(tok_spec, tok_spec), check_vma=False)
```

```python
import numpy as np
import jax
import jax.numpy as jnp
from jax import lax
from jax.experimental import pallas as pl
from jax.experimental.pallas import tpu as pltpu
from jax.sharding import PartitionSpec as P

D_MODEL = 7168
HEADS = 128
Q_LAT = 1536
KV_LAT = 512
ROPE_DIM = 64
NOPE_DIM = 128
V_DIM = 128
QK_DIM = NOPE_DIM + ROPE_DIM
KV_DOWN = KV_LAT + ROPE_DIM
ROPE_BASE = 10000.0
NORM_EPS = 1e-6

ROWS = 16
RING = 4
GROUP = 2 * RING
G_HEADS = HEADS // GROUP
TOKENS = 2048
KV_W = 2 * KV_LAT + 2 * ROPE_DIM
Q_W = KV_LAT + 2 * ROPE_DIM
UNIT = 2 * ROWS
G_ROWS = 2 * RING * UNIT
HALF_N = D_MODEL // 2
OUT_ROWS = 2 * UNIT
K_COLS = G_HEADS * V_DIM
MESH = pl.DeviceIdType.MESH

COLORS = (((0, 256), (2, 1, 0)), ((256, 640), (1, 0, 2)), ((640, 1152), (0, 2, 1)))

W_ROWS = 512
W_SLOTS = 8
N_DOWN = D_MODEL // W_ROWS
N_UP = Q_LAT // W_ROWS
N_OUT = HEADS * V_DIM // W_ROWS
FIRST_OUT = N_DOWN + N_UP
N_CHUNKS = FIRST_OUT + N_OUT
PER_RANK = K_COLS // W_ROWS
KV_SLOTS = 4

ORDER = ((0, 0), (0, 1), (1, 0), (3, 0), (1, 1), (2, 0), (3, 1), (2, 1))


def coords():
    me = lax.axis_index("sp")
    return me // 32, lax.rem(me // 8, 4), lax.rem(me // 2, 4), lax.rem(me, 2)


def device(z, y, x, c):
    return {"sp": ((z * RING + y) * RING + x) * 2 + c}


def shifted(pos, axis, k):
    out = list(pos)
    out[axis] = lax.rem(pos[axis] + k, RING)
    return tuple(out)


def block_kernel(x_one, x_two, gain_q, gain_kv, tab_in, wqd, wkvd, wqu, wkvu, wout, y_one, y_two,
                 xs, qd, kd, kvd_buf, w_buf, wkv, kv_ref, q_ref, tab_ref, q_eff, o_ref, o_all, acc, y_send,
                 w_sem, kvd_sem, wkv_sem, kv_send, kv_recv, r_send, r_recv, d_send, d_recv,
                 q_send, q_recv, t_send, t_recv, dq_send, dq_recv, a_send, a_recv, p_send, p_recv, y_ssem, y_rsem):
    z, y, x, c = coords()
    pos = (z, y, x)
    rank = z * 2 + c
    other = device(z, y, x, 1 - c)
    trans = (((1,), (1,)), ((), ()))

    def rank_at(j):
        out = jnp.int32(0)
        for i, (k, flip) in enumerate(ORDER):
            cc = c if flip == 0 else 1 - c
            out = jnp.where(j == i, lax.rem(z + RING - k, RING) * 2 + cc, out)
        return out

    def down_copy(s):
        slot = lax.rem(s, W_SLOTS)
        return pltpu.make_async_copy(
            wqd.at[pl.ds(pl.multiple_of(s * W_ROWS, W_ROWS), W_ROWS), :], w_buf.at[slot, :, pl.ds(0, Q_LAT)], w_sem.at[slot])

    def up_copy(s):
        slot = lax.rem(s, W_SLOTS)
        width = G_HEADS * QK_DIM
        return pltpu.make_async_copy(
            wqu.at[pl.ds(pl.multiple_of((s - N_DOWN) * W_ROWS, W_ROWS), W_ROWS), pl.ds(pl.multiple_of(rank * width, 128), width)],
            w_buf.at[slot, :, pl.ds(0, width)], w_sem.at[slot])

    def out_copy(s):
        slot = lax.rem(s, W_SLOTS)
        t = s - FIRST_OUT
        row = pl.multiple_of(rank_at(t // PER_RANK) * K_COLS + lax.rem(t, PER_RANK) * W_ROWS, W_ROWS)
        return pltpu.make_async_copy(
            wout.at[pl.ds(row, W_ROWS), pl.ds(pl.multiple_of(c * HALF_N, 128), HALF_N)], w_buf.at[slot], w_sem.at[slot])

    def kvd_copy(s):
        slot = lax.rem(s, KV_SLOTS)
        return pltpu.make_async_copy(
            wkvd.at[:, pl.ds(pl.multiple_of(s * W_ROWS, W_ROWS), W_ROWS)], kvd_buf.at[slot], kvd_sem.at[slot])

    wkv_copy = pltpu.make_async_copy(
        wkvu.at[:, pl.ds(pl.multiple_of(rank * (G_HEADS * 256), 128), G_HEADS * 256)], wkv, wkv_sem)

    for s in range(W_SLOTS):
        down_copy(jnp.int32(s)).start()
        if s < KV_SLOTS:
            kvd_copy(jnp.int32(s)).start()

    barrier = pltpu.get_barrier_semaphore()
    for axis in range(3):
        for k in range(1, RING):
            pl.semaphore_signal(barrier, inc=1, device_id=device(*shifted(pos, axis, k), c), device_id_type=MESH)
    pl.semaphore_signal(barrier, inc=1, device_id=other, device_id_type=MESH)

    xs[:ROWS] = x_one[...]
    xs[ROWS:] = x_two[...]
    tab_ref[:, z, c] = tab_in[...]
    qd[...] = jnp.zeros_like(qd)
    kd[...] = jnp.zeros_like(kd)

    @pl.loop(0, N_DOWN)
    def _(i):
        lhs = xs[:, pl.ds(pl.multiple_of(i * W_ROWS, W_ROWS), W_ROWS)]
        kvd_copy(i).wait()
        kd[:, :KV_DOWN] += lax.dot_general(lhs, kvd_buf[lax.rem(i, KV_SLOTS)], trans, preferred_element_type=jnp.float32)
        down_copy(i).wait()
        qd[...] += jnp.dot(lhs, w_buf[lax.rem(i, W_SLOTS), :, :Q_LAT], preferred_element_type=jnp.float32)

        @pl.when(i + KV_SLOTS < N_DOWN)
        def _():
            kvd_copy(i + KV_SLOTS).start()

        @pl.when(i + W_SLOTS < N_DOWN)
        def _():
            down_copy(i + W_SLOTS).start()

    for s in range(N_DOWN, N_DOWN + W_SLOTS):
        if s < FIRST_OUT:
            up_copy(jnp.int32(s)).start()
        if s == FIRST_OUT:
            wkv_copy.start()
        if s >= FIRST_OUT:
            out_copy(jnp.int32(s)).start()

    lane16 = lax.broadcasted_iota(jnp.int32, (ROWS, 128), 1)
    t0, t1 = tab_in[0], tab_in[1]
    cos2 = jnp.where(lane16 < 32, t0, jnp.where(lane16 < 64, pltpu.roll(t0, 32, 1), jnp.where(lane16 < 96, pltpu.roll(t1, 64, 1), pltpu.roll(t1, 96, 1))))
    sin_hi = jnp.where((lane16 >= 32) & (lane16 < 64), t0, jnp.where(lane16 >= 96, pltpu.roll(t1, 64, 1), 0.0))
    sin_lo = jnp.where(lane16 < 32, -pltpu.roll(t0, 96, 1), jnp.where((lane16 >= 64) & (lane16 < 96), -pltpu.roll(t1, 32, 1), 0.0))
    u = kd[:, :KV_LAT]
    lat = (u * lax.rsqrt(jnp.mean(u * u, axis=-1, keepdims=True) + NORM_EPS) * gain_kv[...]).astype(jnp.bfloat16)
    kv_ref[z, y, x, c, :, 0:KV_LAT] = lat[:ROWS]
    kv_ref[z, y, x, c, :, KV_LAT:2 * KV_LAT] = lat[ROWS:]
    rot = jnp.where(lane16 < 64, kd[:ROWS, KV_LAT:], pltpu.roll(kd[ROWS:, KV_LAT:], 64, 1))
    rot = rot * cos2 + pltpu.roll(rot, 32, 1) * sin_hi + pltpu.roll(rot, 96, 1) * sin_lo
    kv_ref[z, y, x, c, :, 2 * KV_LAT:] = rot.astype(jnp.bfloat16)
    v = qd[...]
    q_lat = (v * lax.rsqrt(jnp.mean(v * v, axis=-1, keepdims=True) + NORM_EPS) * gain_q[...]).astype(jnp.bfloat16)
    q_ref[:, z, c] = q_lat.reshape(2, ROWS, Q_LAT)
    pl.semaphore_wait(barrier, 10)

    def kv_piece(color, phase, at, core, half=None):
        (lo, hi), order = COLORS[color]
        index = [at[0], at[1], at[2]]
        for axis in order[:phase]:
            index[axis] = slice(None)
        if half is not None:
            index[order[0]] = pl.ds(2 * half, 2)
        return kv_ref.at[index[0], index[1], index[2], core, :, pl.ds(lo, hi - lo)]

    def remote(piece, send, recv, to):
        return pltpu.make_async_remote_copy(
            src_ref=piece, dst_ref=piece, send_sem=send, recv_sem=recv, device_id=to, device_id_type=MESH)

    def kv_copy(color, phase, k, at, to):
        return remote(kv_piece(color, phase, at, c), kv_send.at[color, phase, k - 1], kv_recv.at[color, phase, k - 1], to)

    def relay_copy(color, half, at, to):
        return remote(kv_piece(color, 2, at, c, half), r_send.at[color, half], r_recv.at[color, half], to)

    def pass_copy(color, k, at, core):
        return remote(kv_piece(color, 2, at, core), d_send.at[color, k], d_recv.at[color, k], other)

    def q_copy(zz, cc, to, send, recv):
        return remote(q_ref.at[:, zz, cc], send, recv, to)

    def t_copy(zz, cc, to, send, recv):
        return remote(tab_ref.at[:, zz, cc], send, recv, to)

    def start_phase(phase):
        for color in range(3):
            axis = COLORS[color][1][phase]
            for k in (1, 3, 2) if phase < 2 else (1, 3):
                kv_copy(color, phase, k, pos, device(*shifted(pos, axis, k), c)).start()

    def wait_phase(phase):
        for k in (1, 3, 2):
            for color in range(3):
                kv_copy(color, phase, k, shifted(pos, COLORS[color][1][phase], RING - k), other).wait_recv()

    start_phase(0)
    for k in (1, 3, 2):
        to = device(*shifted(pos, 0, k), c)
        t_copy(z, c, to, t_send.at[k - 1], t_recv.at[k - 1]).start()
        q_copy(z, c, to, q_send.at[k - 1], q_recv.at[k - 1]).start()
    t_copy(z, c, other, dq_send.at[0, 0], dq_recv.at[0, 0]).start()
    q_copy(z, c, other, dq_send.at[1, 0], dq_recv.at[1, 0]).start()
    wait_phase(0)
    start_phase(1)
    for k in (1, 3, 2):
        zz = lax.rem(z + RING - k, RING)
        t_copy(zz, c, other, t_send.at[k - 1], t_recv.at[k - 1]).wait_recv()
        t_copy(zz, c, other, dq_send.at[0, k], dq_recv.at[0, k]).start()
        q_copy(zz, c, other, q_send.at[k - 1], q_recv.at[k - 1]).wait_recv()
        q_copy(zz, c, other, dq_send.at[1, k], dq_recv.at[1, k]).start()
    wait_phase(1)
    start_phase(2)
    for color in range(3):
        pass_copy(color, 0, pos, c).start()
    for k in range(RING):
        zz = lax.rem(z + RING - k, RING)
        t_copy(zz, 1 - c, other, dq_send.at[0, k], dq_recv.at[0, k]).wait()
        q_copy(zz, 1 - c, other, dq_send.at[1, k], dq_recv.at[1, k]).wait()

    q2 = q_ref.reshape(G_ROWS, Q_LAT)
    tab2 = tab_ref.reshape(G_ROWS, 128)
    kv2 = kv_ref.reshape(TOKENS, KV_W)
    lane = lax.broadcasted_iota(jnp.int32, (G_ROWS, 128), 1)
    tab = tab2[...]
    cos_t = jnp.where(lane < 32, tab, jnp.where(lane < 64, pltpu.roll(tab, 32, 1), 0.0))
    sin_b = jnp.where((lane >= 32) & (lane < 64), tab, 0.0)
    sin_a = jnp.where(lane < 32, -pltpu.roll(tab, 96, 1), 0.0)

    def put_rope(head, part):
        out = part * cos_t + pltpu.roll(part, 32, 1) * sin_b + pltpu.roll(part, 96, 1) * sin_a
        half = G_ROWS // 2
        out = jnp.concatenate([out[:half], pltpu.roll(out[half:], 64, 1)], axis=0)
        q_eff[:, :, head, :, KV_LAT:] = out.astype(jnp.bfloat16).reshape(2, RING, UNIT, 128)

    def put_nope(head, part):
        w_k = wkv[:, pl.ds(pl.multiple_of(head * 256, 256), 128)]
        out = lax.dot_general(part.astype(jnp.bfloat16), w_k, (((1,), (1,)), ((), ())), preferred_element_type=jnp.float32)
        q_eff[:, :, head, :, :KV_LAT] = out.astype(jnp.bfloat16).reshape(2, RING, UNIT, KV_LAT)

    for s in range(N_DOWN, FIRST_OUT):
        up_copy(jnp.int32(s)).wait()
    wkv_copy.wait()

    def queries(lo, hi):
        @pl.loop(lo, hi)
        def _(p):
            cols = pl.ds(pl.multiple_of(p * (2 * QK_DIM), 128), 2 * QK_DIM)
            f = jnp.zeros((G_ROWS, 2 * QK_DIM), jnp.float32)
            for i in range(N_UP):
                f = f + jnp.dot(q2[:, i * W_ROWS:(i + 1) * W_ROWS], w_buf[(N_DOWN + i) % W_SLOTS, :, cols],
                                preferred_element_type=jnp.float32)
            head = p * 2
            put_nope(head, f[:, :128])
            put_rope(head, f[:, 128:256])
            mid = pltpu.roll(f[:, 128:256], 64, 1)
            last = pltpu.roll(f[:, 256:384], 64, 1)
            put_nope(head + 1, jnp.where(lane < 64, mid, last))
            put_rope(head + 1, last)

    queries(0, G_HEADS // 2)
    for s in range(N_DOWN + W_SLOTS, FIRST_OUT + W_SLOTS):
        out_copy(jnp.int32(s)).start()

    for k in (1, 3):
        for color in range(3):
            axis = COLORS[color][1][2]
            source = shifted(pos, axis, RING - k)
            kv_copy(color, 2, k, source, other).wait_recv()
            relay_copy(color, k // 2, source, device(*shifted(pos, axis, k), c)).start()
            pass_copy(color, k, source, c).start()
    for color in range(3):
        source = shifted(pos, COLORS[color][1][2], 2)
        for half in range(2):
            relay_copy(color, half, source, other).wait_recv()
        pass_copy(color, 2, source, c).start()
    for k in (0, 1, 3, 2):
        for color in range(3):
            pass_copy(color, k, shifted(pos, COLORS[color][1][2], RING - k), 1 - c).wait_recv()

    def ring_copy(mb, k, zz, src_rank, to):
        return pltpu.make_async_remote_copy(
            src_ref=o_ref.at[mb, zz], dst_ref=o_all.at[src_rank, mb], send_sem=a_send.at[mb, k - 1],
            recv_sem=a_recv.at[mb, k - 1], device_id=to, device_id_type=MESH)

    def pair_copy(mb, k, src_rank, src):
        return pltpu.make_async_remote_copy(
            src_ref=src, dst_ref=o_all.at[src_rank, mb], send_sem=p_send.at[mb, k], recv_sem=p_recv.at[mb, k],
            device_id=other, device_id_type=MESH)

    scale2 = (QK_DIM ** -0.5) * 1.4426950408889634
    tok = lax.broadcasted_iota(jnp.int32, (UNIT, 1), 0)

    @pl.loop(0, 2)
    def _(mb):
        lat_cols = pl.ds(pl.multiple_of(mb * KV_LAT, KV_LAT), KV_LAT)
        for zz in range(RING):
            length = (zz + 1) * 512
            key = lax.broadcasted_iota(jnp.int32, (UNIT, length), 1)
            q_tok = zz * 512 + y * 128 + x * 32 + tok
            p0 = tab2[pl.ds(pl.multiple_of((mb * RING + zz) * UNIT, UNIT), UNIT), 64:65].astype(jnp.int32)
            cap = jnp.where((key <= q_tok) & (key >= q_tok - p0), 3e38, -1e30).astype(jnp.float32)
            q = q_eff[mb, zz].reshape(G_HEADS * UNIT, Q_W)
            keys = kv2[:length, lat_cols]
            s = lax.dot_general(q[:, :KV_LAT], keys, trans, preferred_element_type=jnp.float32)
            s = s + lax.dot_general(q[:, KV_LAT:], kv2[:length, 2 * KV_LAT:], trans, preferred_element_type=jnp.float32)
            s = jnp.minimum(s.reshape(G_HEADS, UNIT, length), cap[None])
            top = jnp.max(s, axis=-1, keepdims=True)
            e = jnp.exp2((s - top) * scale2)
            total = jnp.sum(e, axis=-1, keepdims=True)
            e = e.astype(jnp.bfloat16).reshape(G_HEADS * UNIT, length)
            o = jnp.dot(e, keys, preferred_element_type=jnp.float32).reshape(G_HEADS, UNIT, KV_LAT)
            q_eff[mb, zz, :, :, :KV_LAT] = (o / total).astype(jnp.bfloat16)

        @pl.loop(0, G_HEADS)
        def _(h):
            w_v = wkv[:, pl.ds(pl.multiple_of(h * 256 + 128, 128), 128)]
            o_h = jnp.dot(q_eff[mb, :, h, :, :KV_LAT].reshape(RING * UNIT, KV_LAT), w_v, preferred_element_type=jnp.float32)
            o_ref[mb, :, :, :, pl.ds(pl.multiple_of(h * 128, 128), 128)] = o_h.astype(jnp.bfloat16).reshape(RING, 2, ROWS, V_DIM)

        for k in (1, 3, 2):
            zz = lax.rem(z + k, RING)
            ring_copy(mb, k, zz, rank, device(zz, y, x, c)).start()
        pair_copy(mb, 0, rank, o_ref.at[mb, z]).start()

    o_all[rank] = o_ref[:, z]
    acc[...] = jnp.zeros_like(acc)

    @pl.loop(0, N_OUT)
    def _(t):
        for i, (k, flip) in enumerate(ORDER):
            if i == 0:
                continue

            @pl.when(t == i * PER_RANK)
            def _(i=i, k=k, flip=flip):
                src_rank = lax.rem(z + RING - k, RING) * 2 + (c if flip == 0 else 1 - c)
                for mb in range(2):
                    if flip == 0:
                        ring_copy(mb, k, z, src_rank, other).wait_recv()
                        pair_copy(mb, k, src_rank, o_all.at[src_rank, mb]).start()
                    else:
                        pair_copy(mb, k, src_rank, o_all.at[src_rank, mb]).wait_recv()

        s = t + FIRST_OUT
        cols = pl.ds(pl.multiple_of(lax.rem(t, PER_RANK) * W_ROWS, W_ROWS), W_ROWS)
        lhs = o_all[rank_at(t // PER_RANK), :, :, :, cols].reshape(OUT_ROWS, W_ROWS)
        out_copy(s).wait()
        slot = lax.rem(s, W_SLOTS)
        step_n = 512
        for n in range(HALF_N // step_n):
            part = slice(n * step_n, (n + 1) * step_n)
            acc[:, part] += jnp.dot(lhs, w_buf[slot, :, part], preferred_element_type=jnp.float32)

        @pl.when(s + W_SLOTS < N_CHUNKS)
        def _():
            out_copy(s + W_SLOTS).start()

    acc4 = acc.reshape(2, 2, ROWS, HALF_N)
    my_cols = pl.ds(pl.multiple_of(c * HALF_N, 128), HALF_N)
    their_cols = pl.ds(pl.multiple_of((1 - c) * HALF_N, 128), HALF_N)
    outs = (y_one, y_two)

    def y_copy(mb, cols):
        return pltpu.make_async_remote_copy(
            src_ref=y_send.at[mb], dst_ref=outs[mb].at[:, cols], send_sem=y_ssem.at[mb], recv_sem=y_rsem.at[mb],
            device_id=other, device_id_type=MESH)

    for mb in range(2):
        y_send[mb] = acc4[mb, 1 - c].astype(jnp.bfloat16)
    for mb in range(2):
        outs[mb][:, my_cols] = acc4[mb, c].astype(jnp.bfloat16)
    for mb in range(2):
        y_copy(mb, my_cols).start()

    for k in range(1, RING):
        t_copy(z, c, other, t_send.at[k - 1], t_recv.at[k - 1]).wait_send()
        q_copy(z, c, other, q_send.at[k - 1], q_recv.at[k - 1]).wait_send()
        for color in range(3):
            for phase in range(3):
                if phase < 2 or k != 2:
                    kv_copy(color, phase, k, pos, other).wait_send()
    for color in range(3):
        for half in range(2):
            relay_copy(color, half, pos, other).wait_send()
        for k in range(RING):
            pass_copy(color, k, pos, c).wait_send()
    for mb in range(2):
        for k in range(1, RING):
            ring_copy(mb, k, z, rank, other).wait_send()
        for k in range(RING):
            pair_copy(mb, k, rank, o_all.at[rank, mb]).wait_send()
        y_copy(mb, their_cols).wait()


def block(x_one, x_two, gain_q, gain_kv, tab, w_qdown, w_kvdown, w_qup, w_kvup, w_out):
    dma = pltpu.SemaphoreType.DMA
    vmem = pl.BlockSpec(memory_space=pltpu.VMEM)
    hbm = pl.BlockSpec(memory_space=pl.ANY)
    y_shape = jax.ShapeDtypeStruct((ROWS, D_MODEL), jnp.bfloat16)
    bf, f32 = jnp.bfloat16, jnp.float32
    return pl.pallas_call(
        block_kernel,
        out_shape=(y_shape, y_shape),
        in_specs=[vmem] * 5 + [hbm] * 5,
        out_specs=(vmem, vmem),
        scratch_shapes=[
            pltpu.VMEM((2 * ROWS, D_MODEL), bf),
            pltpu.VMEM((2 * ROWS, Q_LAT), f32),
            pltpu.VMEM((2 * ROWS, KV_LAT + 128), f32),
            pltpu.VMEM((KV_SLOTS, KV_DOWN, W_ROWS), bf),
            pltpu.VMEM((W_SLOTS, W_ROWS, HALF_N), bf),
            pltpu.VMEM((KV_LAT, G_HEADS * 256), bf),
            pltpu.VMEM((RING, RING, RING, 2, ROWS, KV_W), bf),
            pltpu.VMEM((2, RING, 2, ROWS, Q_LAT), bf),
            pltpu.VMEM((2, RING, 2, ROWS, 128), f32),
            pltpu.VMEM((2, RING, G_HEADS, UNIT, Q_W), bf),
            pltpu.VMEM((2, RING, 2, ROWS, K_COLS), bf),
            pltpu.VMEM((GROUP, 2, 2, ROWS, K_COLS), bf),
            pltpu.VMEM((OUT_ROWS, HALF_N), f32),
            pltpu.VMEM((2, ROWS, HALF_N), bf),
            dma((W_SLOTS,)), dma((KV_SLOTS,)), dma,
            dma((3, 3, 3)), dma((3, 3, 3)), dma((3, 2)), dma((3, 2)), dma((3, 4)), dma((3, 4)),
            dma((3,)), dma((3,)), dma((3,)), dma((3,)), dma((2, 4)), dma((2, 4)),
            dma((2, 3)), dma((2, 3)), dma((2, 4)), dma((2, 4)), dma((2,)), dma((2,)),
        ],
        compiler_params=pltpu.CompilerParams(collective_id=0, has_side_effects=True, vmem_limit_bytes=67043328),
        name="latent_attention_block",
    )(x_one, x_two, gain_q, gain_kv, tab, w_qdown, w_kvdown, w_qup, w_kvup, w_out)


def tables(pos_one, pos_two):
    lane = np.arange(128)
    inv_freq = (ROPE_BASE ** (-(lane % 32) / (ROPE_DIM // 2))).astype(np.float32)
    pos = jnp.stack([pos_one, pos_two]).astype(jnp.float32)[:, :, None]
    angles = pos * inv_freq
    return jnp.where(lane < 32, jnp.cos(angles), jnp.where(lane < 64, jnp.sin(angles), pos))


def solution(mesh):
    tok_spec = P(('dp', 'sp'), None)
    idx_spec = P(('dp', 'sp'))

    def local_body(x_one, seg_one, pos_one, x_two, seg_two, pos_two, w_qdown, gain_q, w_qup, w_kvdown, gain_kv, w_kvup, w_out):
        gains = (gain_q.astype(jnp.float32)[None], gain_kv.astype(jnp.float32)[None])
        return block(x_one, x_two, *gains, tables(pos_one, pos_two), w_qdown, w_kvdown.T, w_qup, w_kvup, w_out)

    return jax.shard_map(local_body, mesh=mesh, in_specs=(tok_spec, idx_spec, idx_spec, tok_spec, idx_spec, idx_spec, P(), P(), P(), P(), P(), P(), P()), out_specs=(tok_spec, tok_spec), check_vma=False)
```

```python
import jax
import jax.numpy as jnp
from jax import lax
from jax.experimental import pallas as pl
from jax.experimental.pallas import tpu as pltpu
from jax.sharding import PartitionSpec as P

D_MODEL = 7168
HEADS = 128
Q_LAT = 1536
KV_LAT = 512
ROPE_DIM = 64
NOPE_DIM = 128
V_DIM = 128
QK_DIM = NOPE_DIM + ROPE_DIM
KV_DOWN = KV_LAT + ROPE_DIM
ROPE_BASE = 10000.0
NORM_EPS = 1e-6

ROWS = 16
RING = 4
GROUP = 2 * RING
G_HEADS = HEADS // GROUP
TOKENS = 2048
KV_W = 2 * KV_LAT + 2 * ROPE_DIM
Q_W = KV_LAT + 2 * ROPE_DIM
UNIT = 2 * ROWS
G_ROWS = 2 * RING * UNIT
HALF_N = D_MODEL // 2
OUT_ROWS = 2 * UNIT
K_COLS = G_HEADS * V_DIM
MESH = pl.DeviceIdType.MESH

COLORS = (((0, 256), (2, 1, 0)), ((256, 640), (1, 0, 2)), ((640, 1152), (0, 2, 1)))

W_ROWS = 512
W_SLOTS = 8
N_KV = 2
N_DOWN = D_MODEL // W_ROWS
N_UP = Q_LAT // W_ROWS
N_OUT = HEADS * V_DIM // W_ROWS
FIRST_UP = N_KV + N_DOWN
FIRST_OUT = FIRST_UP + N_UP
N_CHUNKS = FIRST_OUT + N_OUT
PER_RANK = K_COLS // W_ROWS

ORDER = ((0, 0), (0, 1), (1, 0), (3, 0), (1, 1), (2, 0), (3, 1), (2, 1))


def coords():
    me = lax.axis_index("sp")
    return me // 32, lax.rem(me // 8, 4), lax.rem(me // 2, 4), lax.rem(me, 2)


def device(z, y, x, c):
    return {"sp": ((z * RING + y) * RING + x) * 2 + c}


def shifted(pos, axis, k):
    out = list(pos)
    out[axis] = lax.rem(pos[axis] + k, RING)
    return tuple(out)


def block_kernel(pos_one, pos_two, gain_q, gain_kv, x_one, x_two, wqd, wkvd, wqu, wkvu, wout, y_ref,
                 xs, qd, kd, kr_buf, w_buf, wkv, kv_ref, q_ref, tab_ref, q_eff, o_ref, o_all, acc, y_send,
                 x_sem, w_sem, kr_sem, wkv_sem, kv_send, kv_recv, r_send, r_recv, d_send, d_recv,
                 q_send, q_recv, t_send, t_recv, dq_send, dq_recv, a_send, a_recv, p_send, p_recv, y_ssem, y_rsem):
    z, y, x, c = coords()
    pos = (z, y, x)
    rank = z * 2 + c
    other = device(z, y, x, 1 - c)
    trans = (((1,), (1,)), ((), ()))

    def rank_at(j):
        out = jnp.int32(0)
        for i, (k, flip) in enumerate(ORDER):
            cc = c if flip == 0 else 1 - c
            out = jnp.where(j == i, lax.rem(z + RING - k, RING) * 2 + cc, out)
        return out

    def x_copy(i):
        return pltpu.make_async_copy((x_one, x_two)[i], xs.at[pl.ds(i * ROWS, ROWS), :], x_sem.at[i])

    def lat_copy(s):
        return pltpu.make_async_copy(wkvd.at[pl.ds(0, KV_LAT), pl.ds(s * HALF_N, HALF_N)], w_buf.at[s], w_sem.at[s])

    def kr_copy(s):
        return pltpu.make_async_copy(
            wkvd.at[pl.ds(KV_LAT, ROPE_DIM), pl.ds(s * HALF_N, HALF_N)], kr_buf.at[s], kr_sem.at[s])

    def down_copy(s):
        slot = lax.rem(s, W_SLOTS)
        return pltpu.make_async_copy(
            wqd.at[pl.ds(pl.multiple_of((s - N_KV) * W_ROWS, W_ROWS), W_ROWS), :], w_buf.at[slot, :, pl.ds(0, Q_LAT)], w_sem.at[slot])

    def up_copy(s):
        slot = lax.rem(s, W_SLOTS)
        width = G_HEADS * QK_DIM
        return pltpu.make_async_copy(
            wqu.at[pl.ds(pl.multiple_of((s - FIRST_UP) * W_ROWS, W_ROWS), W_ROWS), pl.ds(pl.multiple_of(rank * width, 128), width)],
            w_buf.at[slot, :, pl.ds(0, width)], w_sem.at[slot])

    def out_copy(s):
        slot = lax.rem(s, W_SLOTS)
        t = s - FIRST_OUT
        row = pl.multiple_of(rank_at(t // PER_RANK) * K_COLS + lax.rem(t, PER_RANK) * W_ROWS, W_ROWS)
        return pltpu.make_async_copy(
            wout.at[pl.ds(row, W_ROWS), pl.ds(pl.multiple_of(c * HALF_N, 128), HALF_N)], w_buf.at[slot], w_sem.at[slot])

    wkv_copy = pltpu.make_async_copy(
        wkvu.at[:, pl.ds(pl.multiple_of(rank * (G_HEADS * 256), 128), G_HEADS * 256)], wkv, wkv_sem)

    for i in range(2):
        x_copy(i).start()
    for s in range(N_KV):
        lat_copy(s).start()
        kr_copy(s).start()
    for s in range(N_KV, W_SLOTS):
        down_copy(jnp.int32(s)).start()

    barrier = pltpu.get_barrier_semaphore()
    for axis in range(3):
        for k in range(1, RING):
            pl.semaphore_signal(barrier, inc=1, device_id=device(*shifted(pos, axis, k), c), device_id_type=MESH)
    pl.semaphore_signal(barrier, inc=1, device_id=other, device_id_type=MESH)

    row16 = lax.broadcasted_iota(jnp.int32, (ROWS, 128), 0)
    lane16 = lax.broadcasted_iota(jnp.int32, (ROWS, 128), 1)
    freq = jnp.zeros((ROWS, 128), jnp.float32)
    for i in range(ROPE_DIM // 2):
        freq = jnp.where(lax.rem(lane16, ROPE_DIM // 2) == i, ROPE_BASE ** (-i / (ROPE_DIM // 2)), freq)
    tabs = []
    for mb, p_ref in enumerate((pos_one, pos_two)):
        at = jnp.zeros((ROWS, 128), jnp.float32)
        for i in range(ROWS):
            at = jnp.where(row16 == i, p_ref[i].astype(jnp.float32), at)
        angle = at * freq
        tabs.append(jnp.where(lane16 < 32, jnp.cos(angle), jnp.where(lane16 < 64, jnp.sin(angle), at)))
        tab_ref[mb, z, c] = tabs[mb]
    t0, t1 = tabs
    cos2 = jnp.where(lane16 < 32, t0, jnp.where(lane16 < 64, pltpu.roll(t0, 32, 1), jnp.where(lane16 < 96, pltpu.roll(t1, 64, 1), pltpu.roll(t1, 96, 1))))
    sin_hi = jnp.where((lane16 >= 32) & (lane16 < 64), t0, jnp.where(lane16 >= 96, pltpu.roll(t1, 64, 1), 0.0))
    sin_lo = jnp.where(lane16 < 32, -pltpu.roll(t0, 96, 1), jnp.where((lane16 >= 64) & (lane16 < 96), -pltpu.roll(t1, 32, 1), 0.0))

    kd[...] = jnp.zeros_like(kd)
    for i in range(2):
        x_copy(i).wait()
    for s in range(N_KV):
        rhs = xs[:, s * HALF_N:(s + 1) * HALF_N]
        lat_copy(s).wait()
        kd[:KV_LAT, :2 * ROWS] += lax.dot_general(w_buf[s], rhs, trans, preferred_element_type=jnp.float32)
        kr_copy(s).wait()
        kd[KV_LAT:KV_DOWN, :2 * ROWS] += lax.dot_general(kr_buf[s], rhs, trans, preferred_element_type=jnp.float32)
        down_copy(jnp.int32(s + W_SLOTS)).start()
    raw = jnp.transpose(kd[...])[:2 * ROWS]
    u = raw[:, :KV_LAT]
    lat = (u * lax.rsqrt(jnp.mean(u * u, axis=-1, keepdims=True) + NORM_EPS) * gain_kv[...].astype(jnp.float32)[None]).astype(jnp.bfloat16)
    kv_ref[z, y, x, c, :, 0:KV_LAT] = lat[:ROWS]
    kv_ref[z, y, x, c, :, KV_LAT:2 * KV_LAT] = lat[ROWS:]
    rot = jnp.where(lane16 < 64, raw[:ROWS, KV_LAT:], pltpu.roll(raw[ROWS:, KV_LAT:], 64, 1))
    rot = rot * cos2 + pltpu.roll(rot, 32, 1) * sin_hi + pltpu.roll(rot, 96, 1) * sin_lo
    kv_ref[z, y, x, c, :, 2 * KV_LAT:] = rot.astype(jnp.bfloat16)
    qd[...] = jnp.zeros_like(qd)
    pl.semaphore_wait(barrier, 10)

    def q_down(lo, hi):
        @pl.loop(lo, hi)
        def _(i):
            s = i + N_KV
            lhs = xs[:, pl.ds(pl.multiple_of(i * W_ROWS, W_ROWS), W_ROWS)]
            down_copy(s).wait()
            qd[...] += jnp.dot(lhs, w_buf[lax.rem(s, W_SLOTS), :, :Q_LAT], preferred_element_type=jnp.float32)

            @pl.when(s + W_SLOTS < FIRST_UP)
            def _():
                down_copy(s + W_SLOTS).start()

    def kv_piece(color, phase, at, core, half=None):
        (lo, hi), order = COLORS[color]
        index = [at[0], at[1], at[2]]
        for axis in order[:phase]:
            index[axis] = slice(None)
        if half is not None:
            index[order[0]] = pl.ds(2 * half, 2)
        return kv_ref.at[index[0], index[1], index[2], core, :, pl.ds(lo, hi - lo)]

    def remote(piece, send, recv, to):
        return pltpu.make_async_remote_copy(
            src_ref=piece, dst_ref=piece, send_sem=send, recv_sem=recv, device_id=to, device_id_type=MESH)

    def kv_copy(color, phase, k, at, to):
        return remote(kv_piece(color, phase, at, c), kv_send.at[color, phase, k - 1], kv_recv.at[color, phase, k - 1], to)

    def relay_copy(color, half, at, to):
        return remote(kv_piece(color, 2, at, c, half), r_send.at[color, half], r_recv.at[color, half], to)

    def pass_copy(color, k, at, core):
        return remote(kv_piece(color, 2, at, core), d_send.at[color, k], d_recv.at[color, k], other)

    def q_copy(zz, cc, to, send, recv):
        return remote(q_ref.at[:, zz, cc], send, recv, to)

    def t_copy(zz, cc, to, send, recv):
        return remote(tab_ref.at[:, zz, cc], send, recv, to)

    def start_phase(phase):
        for color in range(3):
            axis = COLORS[color][1][phase]
            for k in (1, 3, 2) if phase < 2 else (1, 3):
                kv_copy(color, phase, k, pos, device(*shifted(pos, axis, k), c)).start()

    def wait_phase(phase):
        for k in (1, 3, 2):
            for color in range(3):
                kv_copy(color, phase, k, shifted(pos, COLORS[color][1][phase], RING - k), other).wait_recv()

    start_phase(0)
    q_down(0, N_DOWN // 2)
    wait_phase(0)
    start_phase(1)
    q_down(N_DOWN // 2, N_DOWN)
    for s in range(FIRST_UP, FIRST_UP + W_SLOTS):
        if s < FIRST_OUT:
            up_copy(jnp.int32(s)).start()
        if s == FIRST_OUT:
            wkv_copy.start()
        if s >= FIRST_OUT:
            out_copy(jnp.int32(s)).start()
    v = qd[...]
    q_lat = (v * lax.rsqrt(jnp.mean(v * v, axis=-1, keepdims=True) + NORM_EPS) * gain_q[...].astype(jnp.float32)[None]).astype(jnp.bfloat16)
    q_ref[:, z, c] = q_lat.reshape(2, ROWS, Q_LAT)
    for k in (2, 1, 3):
        to = device(*shifted(pos, 0, k), c)
        t_copy(z, c, to, t_send.at[k - 1], t_recv.at[k - 1]).start()
        q_copy(z, c, to, q_send.at[k - 1], q_recv.at[k - 1]).start()
    t_copy(z, c, other, dq_send.at[0, 0], dq_recv.at[0, 0]).start()
    q_copy(z, c, other, dq_send.at[1, 0], dq_recv.at[1, 0]).start()
    wait_phase(1)
    start_phase(2)
    for color in range(3):
        pass_copy(color, 0, pos, c).start()
    for k in (1, 3, 2):
        zz = lax.rem(z + RING - k, RING)
        t_copy(zz, c, other, t_send.at[k - 1], t_recv.at[k - 1]).wait_recv()
        t_copy(zz, c, other, dq_send.at[0, k], dq_recv.at[0, k]).start()
        q_copy(zz, c, other, q_send.at[k - 1], q_recv.at[k - 1]).wait_recv()
        q_copy(zz, c, other, dq_send.at[1, k], dq_recv.at[1, k]).start()

    for k in (1, 3):
        for color in (1, 2, 0):
            axis = COLORS[color][1][2]
            source = shifted(pos, axis, RING - k)
            kv_copy(color, 2, k, source, other).wait_recv()
            relay_copy(color, k // 2, source, device(*shifted(pos, axis, k), c)).start()
            pass_copy(color, k, source, c).start()
    for k in range(RING):
        zz = lax.rem(z + RING - k, RING)
        t_copy(zz, 1 - c, other, dq_send.at[0, k], dq_recv.at[0, k]).wait()
        q_copy(zz, 1 - c, other, dq_send.at[1, k], dq_recv.at[1, k]).wait()

    q2 = q_ref.reshape(G_ROWS, Q_LAT)
    tab2 = tab_ref.reshape(G_ROWS, 128)
    kv2 = kv_ref.reshape(TOKENS, KV_W)
    lane = lax.broadcasted_iota(jnp.int32, (G_ROWS, 128), 1)
    tab = tab2[...]
    cos_t = jnp.where(lane < 32, tab, jnp.where(lane < 64, pltpu.roll(tab, 32, 1), 0.0))
    sin_b = jnp.where((lane >= 32) & (lane < 64), tab, 0.0)
    sin_a = jnp.where(lane < 32, -pltpu.roll(tab, 96, 1), 0.0)

    def put_rope(head, part):
        out = part * cos_t + pltpu.roll(part, 32, 1) * sin_b + pltpu.roll(part, 96, 1) * sin_a
        half = G_ROWS // 2
        out = jnp.concatenate([out[:half], pltpu.roll(out[half:], 64, 1)], axis=0)
        q_eff[:, :, head, :, KV_LAT:] = out.astype(jnp.bfloat16).reshape(2, RING, UNIT, 128)

    def put_nope(head, part):
        w_k = wkv[:, pl.ds(pl.multiple_of(head * 256, 256), 128)]
        out = lax.dot_general(part.astype(jnp.bfloat16), w_k, (((1,), (1,)), ((), ())), preferred_element_type=jnp.float32)
        q_eff[:, :, head, :, :KV_LAT] = out.astype(jnp.bfloat16).reshape(2, RING, UNIT, KV_LAT)

    for s in range(FIRST_UP, FIRST_OUT):
        up_copy(jnp.int32(s)).wait()
    wkv_copy.wait()

    def queries(lo, hi):
        @pl.loop(lo, hi)
        def _(p):
            cols = pl.ds(pl.multiple_of(p * (2 * QK_DIM), 128), 2 * QK_DIM)
            f = jnp.zeros((G_ROWS, 2 * QK_DIM), jnp.float32)
            for i in range(N_UP):
                f = f + jnp.dot(q2[:, i * W_ROWS:(i + 1) * W_ROWS], w_buf[(FIRST_UP + i) % W_SLOTS, :, cols],
                                preferred_element_type=jnp.float32)
            head = p * 2
            put_nope(head, f[:, :128])
            put_rope(head, f[:, 128:256])
            mid = pltpu.roll(f[:, 128:256], 64, 1)
            last = pltpu.roll(f[:, 256:384], 64, 1)
            put_nope(head + 1, jnp.where(lane < 64, mid, last))
            put_rope(head + 1, last)

    queries(0, G_HEADS // 2)
    for s in range(FIRST_UP + W_SLOTS, FIRST_OUT + W_SLOTS):
        out_copy(jnp.int32(s)).start()

    for color in range(3):
        source = shifted(pos, COLORS[color][1][2], 2)
        for half in range(2):
            relay_copy(color, half, source, other).wait_recv()
        pass_copy(color, 2, source, c).start()
    for k in (0, 1, 3, 2):
        for color in range(3):
            pass_copy(color, k, shifted(pos, COLORS[color][1][2], RING - k), 1 - c).wait_recv()

    def ring_copy(mb, k, zz, src_rank, to):
        return pltpu.make_async_remote_copy(
            src_ref=o_ref.at[mb, zz], dst_ref=o_all.at[src_rank, mb], send_sem=a_send.at[mb, k - 1],
            recv_sem=a_recv.at[mb, k - 1], device_id=to, device_id_type=MESH)

    def pair_copy(mb, k, src_rank, src):
        return pltpu.make_async_remote_copy(
            src_ref=src, dst_ref=o_all.at[src_rank, mb], send_sem=p_send.at[mb, k], recv_sem=p_recv.at[mb, k],
            device_id=other, device_id_type=MESH)

    scale2 = (QK_DIM ** -0.5) * 1.4426950408889634
    tok = lax.broadcasted_iota(jnp.int32, (UNIT, 1), 0)

    @pl.loop(0, 2)
    def _(mb):
        lat_cols = pl.ds(pl.multiple_of(mb * KV_LAT, KV_LAT), KV_LAT)
        for zz in range(RING):
            length = (zz + 1) * 512
            key = lax.broadcasted_iota(jnp.int32, (UNIT, length), 1)
            q_tok = zz * 512 + y * 128 + x * 32 + tok
            p0 = tab2[pl.ds(pl.multiple_of((mb * RING + zz) * UNIT, UNIT), UNIT), 64:65].astype(jnp.int32)
            cap = jnp.where((key <= q_tok) & (key >= q_tok - p0), 3e38, -1e30).astype(jnp.float32)
            q = q_eff[mb, zz].reshape(G_HEADS * UNIT, Q_W)
            keys = kv2[:length, lat_cols]
            s = lax.dot_general(q[:, :KV_LAT], keys, trans, preferred_element_type=jnp.float32)
            s = s + lax.dot_general(q[:, KV_LAT:], kv2[:length, 2 * KV_LAT:], trans, preferred_element_type=jnp.float32)
            s = jnp.minimum(s.reshape(G_HEADS, UNIT, length), cap[None])
            top = jnp.max(s, axis=-1, keepdims=True)
            e = jnp.exp2((s - top) * scale2)
            total = jnp.sum(e, axis=-1, keepdims=True)
            e = e.astype(jnp.bfloat16).reshape(G_HEADS * UNIT, length)
            o = jnp.dot(e, keys, preferred_element_type=jnp.float32).reshape(G_HEADS, UNIT, KV_LAT)
            q_eff[mb, zz, :, :, :KV_LAT] = (o / total).astype(jnp.bfloat16)

        @pl.loop(0, G_HEADS // 4)
        def _(g):
            for i in range(4):
                h = g * 4 + i
                w_v = wkv[:, pl.ds(pl.multiple_of(h * 256 + 128, 128), 128)]
                o_h = jnp.dot(q_eff[mb, :, h, :, :KV_LAT].reshape(RING * UNIT, KV_LAT), w_v, preferred_element_type=jnp.float32)
                o_ref[mb, :, :, :, pl.ds(pl.multiple_of(h * 128, 128), 128)] = o_h.astype(jnp.bfloat16).reshape(RING, 2, ROWS, V_DIM)

        for k in (1, 3, 2):
            zz = lax.rem(z + k, RING)
            ring_copy(mb, k, zz, rank, device(zz, y, x, c)).start()
        pair_copy(mb, 0, rank, o_ref.at[mb, z]).start()

    o_all[rank] = o_ref[:, z]
    acc[...] = jnp.zeros_like(acc)

    @pl.loop(0, N_OUT)
    def _(t):
        for i, (k, flip) in enumerate(ORDER):
            if i == 0:
                continue

            @pl.when(t == i * PER_RANK)
            def _(i=i, k=k, flip=flip):
                src_rank = lax.rem(z + RING - k, RING) * 2 + (c if flip == 0 else 1 - c)
                for mb in range(2):
                    if flip == 0:
                        ring_copy(mb, k, z, src_rank, other).wait_recv()
                        pair_copy(mb, k, src_rank, o_all.at[src_rank, mb]).start()
                    else:
                        pair_copy(mb, k, src_rank, o_all.at[src_rank, mb]).wait_recv()

        s = t + FIRST_OUT
        cols = pl.ds(pl.multiple_of(lax.rem(t, PER_RANK) * W_ROWS, W_ROWS), W_ROWS)
        lhs = o_all[rank_at(t // PER_RANK), :, :, :, cols].reshape(OUT_ROWS, W_ROWS)
        out_copy(s).wait()
        slot = lax.rem(s, W_SLOTS)
        step_n = 512
        for n in range(HALF_N // step_n):
            part = slice(n * step_n, (n + 1) * step_n)
            acc[:, part] += jnp.dot(lhs, w_buf[slot, :, part], preferred_element_type=jnp.float32)

        @pl.when(s + W_SLOTS < N_CHUNKS)
        def _():
            out_copy(s + W_SLOTS).start()

    acc4 = acc.reshape(2, 2, ROWS, HALF_N)
    my_cols = pl.ds(pl.multiple_of(c * HALF_N, 128), HALF_N)
    their_cols = pl.ds(pl.multiple_of((1 - c) * HALF_N, 128), HALF_N)
    outs = (y_ref.at[0], y_ref.at[1])

    def y_copy(mb, cols):
        return pltpu.make_async_remote_copy(
            src_ref=y_send.at[mb], dst_ref=outs[mb].at[:, cols], send_sem=y_ssem.at[mb], recv_sem=y_rsem.at[mb],
            device_id=other, device_id_type=MESH)

    for mb in range(2):
        y_send[mb] = acc4[mb, 1 - c].astype(jnp.bfloat16)
    for mb in range(2):
        outs[mb][:, my_cols] = acc4[mb, c].astype(jnp.bfloat16)
    for mb in range(2):
        y_copy(mb, my_cols).start()

    for k in range(1, RING):
        t_copy(z, c, other, t_send.at[k - 1], t_recv.at[k - 1]).wait_send()
        q_copy(z, c, other, q_send.at[k - 1], q_recv.at[k - 1]).wait_send()
        for color in range(3):
            for phase in range(3):
                if phase < 2 or k != 2:
                    kv_copy(color, phase, k, pos, other).wait_send()
    for color in range(3):
        for half in range(2):
            relay_copy(color, half, pos, other).wait_send()
        for k in range(RING):
            pass_copy(color, k, pos, c).wait_send()
    for mb in range(2):
        for k in range(1, RING):
            ring_copy(mb, k, z, rank, other).wait_send()
        for k in range(RING):
            pair_copy(mb, k, rank, o_all.at[rank, mb]).wait_send()
        y_copy(mb, their_cols).wait()


def copy_kernel(y_ref, y_one, y_two):
    y_one[...] = y_ref[0]
    y_two[...] = y_ref[1]


def block(pos_one, pos_two, gain_q, gain_kv, x_one, x_two, w_qdown, w_kvdown, w_qup, w_kvup, w_out):
    dma = pltpu.SemaphoreType.DMA
    vmem = pl.BlockSpec(memory_space=pltpu.VMEM)
    smem = pl.BlockSpec(memory_space=pltpu.SMEM)
    hbm = pl.BlockSpec(memory_space=pl.ANY)
    bf, f32 = jnp.bfloat16, jnp.float32
    y = pl.pallas_call(
        block_kernel,
        out_shape=jax.ShapeDtypeStruct((2, ROWS, D_MODEL), bf),
        in_specs=[smem] * 2 + [vmem] * 2 + [hbm] * 7,
        out_specs=vmem,
        scratch_shapes=[
            pltpu.VMEM((2 * ROWS, D_MODEL), bf),
            pltpu.VMEM((2 * ROWS, Q_LAT), f32),
            pltpu.VMEM((KV_LAT + 128, 128), f32),
            pltpu.VMEM((N_KV, ROPE_DIM, HALF_N), bf),
            pltpu.VMEM((W_SLOTS, W_ROWS, HALF_N), bf),
            pltpu.VMEM((KV_LAT, G_HEADS * 256), bf),
            pltpu.VMEM((RING, RING, RING, 2, ROWS, KV_W), bf),
            pltpu.VMEM((2, RING, 2, ROWS, Q_LAT), bf),
            pltpu.VMEM((2, RING, 2, ROWS, 128), f32),
            pltpu.VMEM((2, RING, G_HEADS, UNIT, Q_W), bf),
            pltpu.VMEM((2, RING, 2, ROWS, K_COLS), bf),
            pltpu.VMEM((GROUP, 2, 2, ROWS, K_COLS), bf),
            pltpu.VMEM((OUT_ROWS, HALF_N), f32),
            pltpu.VMEM((2, ROWS, HALF_N), bf),
            dma((2,)), dma((W_SLOTS,)), dma((N_KV,)), dma,
            dma((3, 3, 3)), dma((3, 3, 3)), dma((3, 2)), dma((3, 2)), dma((3, 4)), dma((3, 4)),
            dma((3,)), dma((3,)), dma((3,)), dma((3,)), dma((2, 4)), dma((2, 4)),
            dma((2, 3)), dma((2, 3)), dma((2, 4)), dma((2, 4)), dma((2,)), dma((2,)),
        ],
        compiler_params=pltpu.CompilerParams(collective_id=0, has_side_effects=True, vmem_limit_bytes=67043328),
        name="latent_attention_block",
    )(pos_one, pos_two, gain_q, gain_kv, x_one, x_two, w_qdown, w_kvdown, w_qup, w_kvup, w_out)
    y_shape = jax.ShapeDtypeStruct((ROWS, D_MODEL), bf)
    return pl.pallas_call(copy_kernel, out_shape=(y_shape, y_shape), in_specs=[vmem], out_specs=(vmem, vmem), name="results")(y)


def solution(mesh):
    tok_spec = P(('dp', 'sp'), None)
    idx_spec = P(('dp', 'sp'))

    def local_body(x_one, seg_one, pos_one, x_two, seg_two, pos_two, w_qdown, gain_q, w_qup, w_kvdown, gain_kv, w_kvup, w_out):
        return block(pos_one, pos_two, gain_q, gain_kv, x_one, x_two, w_qdown, w_kvdown.T, w_qup, w_kvup, w_out)

    return jax.shard_map(local_body, mesh=mesh, in_specs=(tok_spec, idx_spec, idx_spec, tok_spec, idx_spec, idx_spec, P(), P(), P(), P(), P(), P(), P()), out_specs=(tok_spec, tok_spec), check_vma=False)
```

```python
import jax
import jax.numpy as jnp
from jax import lax
from jax.experimental import pallas as pl
from jax.experimental.pallas import tpu as pltpu
from jax.sharding import PartitionSpec as P

D_MODEL = 7168
HEADS = 128
Q_LAT = 1536
KV_LAT = 512
ROPE_DIM = 64
NOPE_DIM = 128
V_DIM = 128
QK_DIM = NOPE_DIM + ROPE_DIM
KV_DOWN = KV_LAT + ROPE_DIM
ROPE_BASE = 10000.0
NORM_EPS = 1e-6

ROWS = 16
RING = 4
GROUP = 2 * RING
G_HEADS = HEADS // GROUP
TOKENS = 2048
KV_W = 2 * KV_LAT + 2 * ROPE_DIM
Q_W = KV_LAT + 2 * ROPE_DIM
UNIT = 2 * ROWS
G_ROWS = 2 * RING * UNIT
HALF_N = D_MODEL // 2
OUT_ROWS = 2 * UNIT
K_COLS = G_HEADS * V_DIM
MESH = pl.DeviceIdType.MESH

COLORS = (((0, 256), (2, 1, 0)), ((256, 640), (1, 0, 2)), ((640, 1152), (0, 2, 1)))

W_ROWS = 512
W_SLOTS = 9
N_KV = 2
N_DOWN = D_MODEL // W_ROWS
N_UP = Q_LAT // W_ROWS
N_OUT = HEADS * V_DIM // W_ROWS
FIRST_UP = N_KV + N_DOWN
FIRST_OUT = FIRST_UP + N_UP
N_CHUNKS = FIRST_OUT + N_OUT
PER_RANK = K_COLS // W_ROWS

ORDER = ((0, 0), (0, 1), (1, 0), (3, 0), (1, 1), (2, 0), (3, 1), (2, 1))


def coords():
    me = lax.axis_index("sp")
    return me // 32, lax.rem(me // 8, 4), lax.rem(me // 2, 4), lax.rem(me, 2)


def device(z, y, x, c):
    return {"sp": ((z * RING + y) * RING + x) * 2 + c}


def shifted(pos, axis, k):
    out = list(pos)
    out[axis] = lax.rem(pos[axis] + k, RING)
    return tuple(out)


def block_kernel(pos_one, pos_two, gain_q, gain_kv, x_one, x_two, wqd, wkvd, wqu, wkvu, wout, y_ref,
                 xs, qd, kd, kr_buf, w_buf, wkv, kv_ref, q_ref, tab_ref, q_eff, o_ref, o_all, acc, y_send,
                 x_sem, w_sem, kr_sem, wkv_sem, kv_send, kv_recv, r_send, r_recv, d_send, d_recv,
                 q_send, q_recv, t_send, t_recv, dq_send, dq_recv, a_send, a_recv, p_send, p_recv, y_ssem, y_rsem):
    z, y, x, c = coords()
    pos = (z, y, x)
    rank = z * 2 + c
    other = device(z, y, x, 1 - c)
    trans = (((1,), (1,)), ((), ()))

    def rank_at(j):
        out = jnp.int32(0)
        for i, (k, flip) in enumerate(ORDER):
            cc = c if flip == 0 else 1 - c
            out = jnp.where(j == i, lax.rem(z + RING - k, RING) * 2 + cc, out)
        return out

    def x_copy(i):
        return pltpu.make_async_copy((x_one, x_two)[i], xs.at[pl.ds(i * ROWS, ROWS), :], x_sem.at[i])

    def lat_copy(s):
        return pltpu.make_async_copy(wkvd.at[pl.ds(0, KV_LAT), pl.ds(s * HALF_N, HALF_N)], w_buf.at[s], w_sem.at[s])

    def kr_copy(s):
        return pltpu.make_async_copy(
            wkvd.at[pl.ds(KV_LAT, ROPE_DIM), pl.ds(s * HALF_N, HALF_N)], kr_buf.at[s], kr_sem.at[s])

    def down_copy(s):
        slot = lax.rem(s, W_SLOTS)
        return pltpu.make_async_copy(
            wqd.at[pl.ds(pl.multiple_of((s - N_KV) * W_ROWS, W_ROWS), W_ROWS), :], w_buf.at[slot, :, pl.ds(0, Q_LAT)], w_sem.at[slot])

    def up_copy(s):
        slot = lax.rem(s, W_SLOTS)
        width = G_HEADS * QK_DIM
        return pltpu.make_async_copy(
            wqu.at[pl.ds(pl.multiple_of((s - FIRST_UP) * W_ROWS, W_ROWS), W_ROWS), pl.ds(pl.multiple_of(rank * width, 128), width)],
            w_buf.at[slot, :, pl.ds(0, width)], w_sem.at[slot])

    def out_copy(s):
        slot = lax.rem(s, W_SLOTS)
        t = s - FIRST_OUT
        row = pl.multiple_of(rank_at(t // PER_RANK) * K_COLS + lax.rem(t, PER_RANK) * W_ROWS, W_ROWS)
        return pltpu.make_async_copy(
            wout.at[pl.ds(row, W_ROWS), pl.ds(pl.multiple_of(c * HALF_N, 128), HALF_N)], w_buf.at[slot], w_sem.at[slot])

    wkv_copy = pltpu.make_async_copy(
        wkvu.at[:, pl.ds(pl.multiple_of(rank * (G_HEADS * 256), 128), G_HEADS * 256)], wkv, wkv_sem)

    for i in range(2):
        x_copy(i).start()
    for s in range(N_KV):
        lat_copy(s).start()
        kr_copy(s).start()
    down_copy(jnp.int32(N_KV)).start()

    barrier = pltpu.get_barrier_semaphore()
    for axis in range(3):
        for k in range(1, RING):
            pl.semaphore_signal(barrier, inc=1, device_id=device(*shifted(pos, axis, k), c), device_id_type=MESH)
    pl.semaphore_signal(barrier, inc=1, device_id=other, device_id_type=MESH)

    row16 = lax.broadcasted_iota(jnp.int32, (ROWS, 128), 0)
    lane16 = lax.broadcasted_iota(jnp.int32, (ROWS, 128), 1)
    freq = jnp.zeros((ROWS, 128), jnp.float32)
    for i in range(ROPE_DIM // 2):
        freq = jnp.where(lax.rem(lane16, ROPE_DIM // 2) == i, ROPE_BASE ** (-i / (ROPE_DIM // 2)), freq)
    tabs = []
    for mb, p_ref in enumerate((pos_one, pos_two)):
        at = jnp.zeros((ROWS, 128), jnp.float32)
        for i in range(ROWS):
            at = jnp.where(row16 == i, p_ref[i].astype(jnp.float32), at)
        angle = at * freq
        tabs.append(jnp.where(lane16 < 32, jnp.cos(angle), jnp.where(lane16 < 64, jnp.sin(angle), at)))
        tab_ref[mb, z, c] = tabs[mb]
    t0, t1 = tabs
    cos2 = jnp.where(lane16 < 32, t0, jnp.where(lane16 < 64, pltpu.roll(t0, 32, 1), jnp.where(lane16 < 96, pltpu.roll(t1, 64, 1), pltpu.roll(t1, 96, 1))))
    sin_hi = jnp.where((lane16 >= 32) & (lane16 < 64), t0, jnp.where(lane16 >= 96, pltpu.roll(t1, 64, 1), 0.0))
    sin_lo = jnp.where(lane16 < 32, -pltpu.roll(t0, 96, 1), jnp.where((lane16 >= 64) & (lane16 < 96), -pltpu.roll(t1, 32, 1), 0.0))

    kd[...] = jnp.zeros_like(kd)
    for i in range(2):
        x_copy(i).wait()
    for s in range(N_KV):
        rhs = xs[:, s * HALF_N:(s + 1) * HALF_N]
        lat_copy(s).wait()
        if s == 0:
            for i in range(N_KV + 1, W_SLOTS):
                down_copy(jnp.int32(i)).start()
        kd[:KV_LAT, :2 * ROWS] += lax.dot_general(w_buf[s], rhs, trans, preferred_element_type=jnp.float32)
        kr_copy(s).wait()
        kd[KV_LAT:KV_DOWN, :2 * ROWS] += lax.dot_general(kr_buf[s], rhs, trans, preferred_element_type=jnp.float32)
        down_copy(jnp.int32(s + W_SLOTS)).start()
    raw = jnp.transpose(kd[...])[:2 * ROWS]
    u = raw[:, :KV_LAT]
    lat = (u * lax.rsqrt(jnp.mean(u * u, axis=-1, keepdims=True) + NORM_EPS) * gain_kv[...].astype(jnp.float32)[None]).astype(jnp.bfloat16)
    kv_ref[z, y, x, c, :, 0:KV_LAT] = lat[:ROWS]
    kv_ref[z, y, x, c, :, KV_LAT:2 * KV_LAT] = lat[ROWS:]
    rot = jnp.where(lane16 < 64, raw[:ROWS, KV_LAT:], pltpu.roll(raw[ROWS:, KV_LAT:], 64, 1))
    rot = rot * cos2 + pltpu.roll(rot, 32, 1) * sin_hi + pltpu.roll(rot, 96, 1) * sin_lo
    kv_ref[z, y, x, c, :, 2 * KV_LAT:] = rot.astype(jnp.bfloat16)
    qd[...] = jnp.zeros_like(qd)
    pl.semaphore_wait(barrier, 10)

    def q_down(lo, hi):
        @pl.loop(lo, hi)
        def _(i):
            s = i + N_KV
            lhs = xs[:, pl.ds(pl.multiple_of(i * W_ROWS, W_ROWS), W_ROWS)]
            down_copy(s).wait()
            qd[...] += jnp.dot(lhs, w_buf[lax.rem(s, W_SLOTS), :, :Q_LAT], preferred_element_type=jnp.float32)

            @pl.when(s + W_SLOTS < FIRST_UP)
            def _():
                down_copy(s + W_SLOTS).start()

    def kv_piece(color, phase, at, core, half=None):
        (lo, hi), order = COLORS[color]
        index = [at[0], at[1], at[2]]
        for axis in order[:phase]:
            index[axis] = slice(None)
        if half is not None:
            index[order[0]] = pl.ds(2 * half, 2)
        return kv_ref.at[index[0], index[1], index[2], core, :, pl.ds(lo, hi - lo)]

    def remote(piece, send, recv, to):
        return pltpu.make_async_remote_copy(
            src_ref=piece, dst_ref=piece, send_sem=send, recv_sem=recv, device_id=to, device_id_type=MESH)

    def kv_copy(color, phase, k, at, to):
        return remote(kv_piece(color, phase, at, c), kv_send.at[color, phase, k - 1], kv_recv.at[color, phase, k - 1], to)

    def relay_copy(color, half, at, to):
        return remote(kv_piece(color, 2, at, c, half), r_send.at[color, half], r_recv.at[color, half], to)

    def pass_copy(color, k, at, core):
        return remote(kv_piece(color, 2, at, core), d_send.at[color, k], d_recv.at[color, k], other)

    def q_copy(zz, cc, to, send, recv):
        return remote(q_ref.at[:, zz, cc], send, recv, to)

    def t_copy(zz, cc, to, send, recv):
        return remote(tab_ref.at[:, zz, cc], send, recv, to)

    def start_phase(phase):
        for color in range(3):
            axis = COLORS[color][1][phase]
            for k in (1, 3, 2) if phase < 2 else (1, 3):
                kv_copy(color, phase, k, pos, device(*shifted(pos, axis, k), c)).start()

    def wait_phase(phase):
        for k in (1, 3, 2):
            for color in range(3):
                kv_copy(color, phase, k, shifted(pos, COLORS[color][1][phase], RING - k), other).wait_recv()

    start_phase(0)
    q_down(0, N_DOWN // 2)
    wait_phase(0)
    start_phase(1)
    q_down(N_DOWN // 2, N_DOWN)
    for s in range(FIRST_UP, FIRST_UP + W_SLOTS):
        if s < FIRST_OUT:
            up_copy(jnp.int32(s)).start()
        if s == FIRST_OUT:
            wkv_copy.start()
        if s >= FIRST_OUT:
            out_copy(jnp.int32(s)).start()
    v = qd[...]
    q_lat = (v * lax.rsqrt(jnp.mean(v * v, axis=-1, keepdims=True) + NORM_EPS) * gain_q[...].astype(jnp.float32)[None]).astype(jnp.bfloat16)
    q_ref[:, z, c] = q_lat.reshape(2, ROWS, Q_LAT)
    for k in (2, 1, 3):
        to = device(*shifted(pos, 0, k), c)
        t_copy(z, c, to, t_send.at[k - 1], t_recv.at[k - 1]).start()
        q_copy(z, c, to, q_send.at[k - 1], q_recv.at[k - 1]).start()
    t_copy(z, c, other, dq_send.at[0, 0], dq_recv.at[0, 0]).start()
    q_copy(z, c, other, dq_send.at[1, 0], dq_recv.at[1, 0]).start()
    wait_phase(1)
    start_phase(2)
    for color in range(3):
        pass_copy(color, 0, pos, c).start()
    for k in (1, 3, 2):
        zz = lax.rem(z + RING - k, RING)
        t_copy(zz, c, other, t_send.at[k - 1], t_recv.at[k - 1]).wait_recv()
        t_copy(zz, c, other, dq_send.at[0, k], dq_recv.at[0, k]).start()
        q_copy(zz, c, other, q_send.at[k - 1], q_recv.at[k - 1]).wait_recv()
        q_copy(zz, c, other, dq_send.at[1, k], dq_recv.at[1, k]).start()

    for k in (1, 3):
        for color in (1, 2, 0):
            axis = COLORS[color][1][2]
            source = shifted(pos, axis, RING - k)
            kv_copy(color, 2, k, source, other).wait_recv()
            relay_copy(color, k // 2, source, device(*shifted(pos, axis, k), c)).start()
            pass_copy(color, k, source, c).start()
    for k in range(RING):
        zz = lax.rem(z + RING - k, RING)
        t_copy(zz, 1 - c, other, dq_send.at[0, k], dq_recv.at[0, k]).wait()
        q_copy(zz, 1 - c, other, dq_send.at[1, k], dq_recv.at[1, k]).wait()

    q2 = q_ref.reshape(G_ROWS, Q_LAT)
    tab2 = tab_ref.reshape(G_ROWS, 128)
    kv2 = kv_ref.reshape(TOKENS, KV_W)
    lane = lax.broadcasted_iota(jnp.int32, (G_ROWS, 128), 1)
    tab = tab2[...]
    cos_t = jnp.where(lane < 32, tab, jnp.where(lane < 64, pltpu.roll(tab, 32, 1), 0.0))
    sin_b = jnp.where((lane >= 32) & (lane < 64), tab, 0.0)
    sin_a = jnp.where(lane < 32, -pltpu.roll(tab, 96, 1), 0.0)

    def put_rope(head, part):
        out = part * cos_t + pltpu.roll(part, 32, 1) * sin_b + pltpu.roll(part, 96, 1) * sin_a
        half = G_ROWS // 2
        out = jnp.concatenate([out[:half], pltpu.roll(out[half:], 64, 1)], axis=0)
        q_eff[:, :, head, :, KV_LAT:] = out.astype(jnp.bfloat16).reshape(2, RING, UNIT, 128)

    def put_nope(head, part):
        w_k = wkv[:, pl.ds(pl.multiple_of(head * 256, 256), 128)]
        out = lax.dot_general(part.astype(jnp.bfloat16), w_k, (((1,), (1,)), ((), ())), preferred_element_type=jnp.float32)
        q_eff[:, :, head, :, :KV_LAT] = out.astype(jnp.bfloat16).reshape(2, RING, UNIT, KV_LAT)

    for s in range(FIRST_UP, FIRST_OUT):
        up_copy(jnp.int32(s)).wait()
    wkv_copy.wait()

    def queries(lo, hi):
        @pl.loop(lo, hi)
        def _(g):
            parts = []
            for i in range(2):
                cols = pl.ds(pl.multiple_of((2 * g + i) * (2 * QK_DIM), 128), 2 * QK_DIM)
                f = jnp.zeros((G_ROWS, 2 * QK_DIM), jnp.float32)
                for n in range(N_UP):
                    f = f + jnp.dot(q2[:, n * W_ROWS:(n + 1) * W_ROWS], w_buf[(FIRST_UP + n) % W_SLOTS, :, cols],
                                    preferred_element_type=jnp.float32)
                parts.append(f)
            for i, f in enumerate(parts):
                head = 4 * g + 2 * i
                put_nope(head, f[:, :128])
                put_rope(head, f[:, 128:256])
                mid = pltpu.roll(f[:, 128:256], 64, 1)
                last = pltpu.roll(f[:, 256:384], 64, 1)
                put_nope(head + 1, jnp.where(lane < 64, mid, last))
                put_rope(head + 1, last)

    queries(0, G_HEADS // 4)
    for s in range(FIRST_UP + W_SLOTS, FIRST_OUT + W_SLOTS):
        out_copy(jnp.int32(s)).start()

    for color in range(3):
        source = shifted(pos, COLORS[color][1][2], 2)
        for half in range(2):
            relay_copy(color, half, source, other).wait_recv()
        pass_copy(color, 2, source, c).start()
    for k in (0, 1, 3, 2):
        for color in range(3):
            pass_copy(color, k, shifted(pos, COLORS[color][1][2], RING - k), 1 - c).wait_recv()

    def ring_copy(mb, k, zz, src_rank, to):
        return pltpu.make_async_remote_copy(
            src_ref=o_ref.at[mb, zz], dst_ref=o_all.at[src_rank, mb], send_sem=a_send.at[mb, k - 1],
            recv_sem=a_recv.at[mb, k - 1], device_id=to, device_id_type=MESH)

    def pair_copy(mb, k, src_rank, src):
        return pltpu.make_async_remote_copy(
            src_ref=src, dst_ref=o_all.at[src_rank, mb], send_sem=p_send.at[mb, k], recv_sem=p_recv.at[mb, k],
            device_id=other, device_id_type=MESH)

    scale2 = (QK_DIM ** -0.5) * 1.4426950408889634
    tok = lax.broadcasted_iota(jnp.int32, (UNIT, 1), 0)

    @pl.loop(0, 2)
    def _(mb):
        lat_cols = pl.ds(pl.multiple_of(mb * KV_LAT, KV_LAT), KV_LAT)
        for zz in range(RING):
            length = (zz + 1) * 512
            key = lax.broadcasted_iota(jnp.int32, (UNIT, length), 1)
            q_tok = zz * 512 + y * 128 + x * 32 + tok
            p0 = tab2[pl.ds(pl.multiple_of((mb * RING + zz) * UNIT, UNIT), UNIT), 64:65].astype(jnp.int32)
            cap = jnp.where((key <= q_tok) & (key >= q_tok - p0), 3e38, -1e30).astype(jnp.float32)
            q = q_eff[mb, zz].reshape(G_HEADS * UNIT, Q_W)
            keys = kv2[:length, lat_cols]
            s = lax.dot_general(q[:, :KV_LAT], keys, trans, preferred_element_type=jnp.float32)
            s = s + lax.dot_general(q[:, KV_LAT:], kv2[:length, 2 * KV_LAT:], trans, preferred_element_type=jnp.float32)
            s = jnp.minimum(s.reshape(G_HEADS, UNIT, length), cap[None])
            top = jnp.max(s, axis=-1, keepdims=True)
            e = jnp.exp2((s - top) * scale2)
            total = jnp.sum(e, axis=-1, keepdims=True)
            e = e.astype(jnp.bfloat16).reshape(G_HEADS * UNIT, length)
            o = jnp.dot(e, keys, preferred_element_type=jnp.float32).reshape(G_HEADS, UNIT, KV_LAT)
            q_eff[mb, zz, :, :, :KV_LAT] = (o / total).astype(jnp.bfloat16)

        @pl.loop(0, G_HEADS // 4)
        def _(g):
            for i in range(4):
                h = g * 4 + i
                w_v = wkv[:, pl.ds(pl.multiple_of(h * 256 + 128, 128), 128)]
                o_h = jnp.dot(q_eff[mb, :, h, :, :KV_LAT].reshape(RING * UNIT, KV_LAT), w_v, preferred_element_type=jnp.float32)
                o_ref[mb, :, :, :, pl.ds(pl.multiple_of(h * 128, 128), 128)] = o_h.astype(jnp.bfloat16).reshape(RING, 2, ROWS, V_DIM)

        for k in (1, 3, 2):
            zz = lax.rem(z + k, RING)
            ring_copy(mb, k, zz, rank, device(zz, y, x, c)).start()
        pair_copy(mb, 0, rank, o_ref.at[mb, z]).start()

    o_all[rank] = o_ref[:, z]
    acc[...] = jnp.zeros_like(acc)

    @pl.loop(0, N_OUT)
    def _(t):
        for i, (k, flip) in enumerate(ORDER):
            if i == 0:
                continue

            @pl.when(t == i * PER_RANK)
            def _(i=i, k=k, flip=flip):
                src_rank = lax.rem(z + RING - k, RING) * 2 + (c if flip == 0 else 1 - c)
                for mb in range(2):
                    if flip == 0:
                        ring_copy(mb, k, z, src_rank, other).wait_recv()
                        pair_copy(mb, k, src_rank, o_all.at[src_rank, mb]).start()
                    else:
                        pair_copy(mb, k, src_rank, o_all.at[src_rank, mb]).wait_recv()

        s = t + FIRST_OUT
        cols = pl.ds(pl.multiple_of(lax.rem(t, PER_RANK) * W_ROWS, W_ROWS), W_ROWS)
        lhs = o_all[rank_at(t // PER_RANK), :, :, :, cols].reshape(OUT_ROWS, W_ROWS)
        out_copy(s).wait()
        slot = lax.rem(s, W_SLOTS)
        step_n = 512
        for n in range(HALF_N // step_n):
            part = slice(n * step_n, (n + 1) * step_n)
            acc[:, part] += jnp.dot(lhs, w_buf[slot, :, part], preferred_element_type=jnp.float32)

        @pl.when(s + W_SLOTS < N_CHUNKS)
        def _():
            out_copy(s + W_SLOTS).start()

    acc4 = acc.reshape(2, 2, ROWS, HALF_N)
    my_cols = pl.ds(pl.multiple_of(c * HALF_N, 128), HALF_N)
    their_cols = pl.ds(pl.multiple_of((1 - c) * HALF_N, 128), HALF_N)
    outs = (y_ref.at[0], y_ref.at[1])

    def y_copy(mb, cols):
        return pltpu.make_async_remote_copy(
            src_ref=y_send.at[mb], dst_ref=outs[mb].at[:, cols], send_sem=y_ssem.at[mb], recv_sem=y_rsem.at[mb],
            device_id=other, device_id_type=MESH)

    for mb in range(2):
        y_send[mb] = acc4[mb, 1 - c].astype(jnp.bfloat16)
    for mb in range(2):
        outs[mb][:, my_cols] = acc4[mb, c].astype(jnp.bfloat16)
    for mb in range(2):
        y_copy(mb, my_cols).start()

    for k in range(1, RING):
        t_copy(z, c, other, t_send.at[k - 1], t_recv.at[k - 1]).wait_send()
        q_copy(z, c, other, q_send.at[k - 1], q_recv.at[k - 1]).wait_send()
        for color in range(3):
            for phase in range(3):
                if phase < 2 or k != 2:
                    kv_copy(color, phase, k, pos, other).wait_send()
    for color in range(3):
        for half in range(2):
            relay_copy(color, half, pos, other).wait_send()
        for k in range(RING):
            pass_copy(color, k, pos, c).wait_send()
    for mb in range(2):
        for k in range(1, RING):
            ring_copy(mb, k, z, rank, other).wait_send()
        for k in range(RING):
            pair_copy(mb, k, rank, o_all.at[rank, mb]).wait_send()
        y_copy(mb, their_cols).wait()


def copy_kernel(y_ref, y_one, y_two):
    y_one[...] = y_ref[0]
    y_two[...] = y_ref[1]


def block(pos_one, pos_two, gain_q, gain_kv, x_one, x_two, w_qdown, w_kvdown, w_qup, w_kvup, w_out):
    dma = pltpu.SemaphoreType.DMA
    vmem = pl.BlockSpec(memory_space=pltpu.VMEM)
    smem = pl.BlockSpec(memory_space=pltpu.SMEM)
    hbm = pl.BlockSpec(memory_space=pl.ANY)
    bf, f32 = jnp.bfloat16, jnp.float32
    y = pl.pallas_call(
        block_kernel,
        out_shape=jax.ShapeDtypeStruct((2, ROWS, D_MODEL), bf),
        in_specs=[smem] * 2 + [vmem] * 2 + [hbm] * 7,
        out_specs=vmem,
        scratch_shapes=[
            pltpu.VMEM((2 * ROWS, D_MODEL), bf),
            pltpu.VMEM((2 * ROWS, Q_LAT), f32),
            pltpu.VMEM((KV_LAT + 128, 128), f32),
            pltpu.VMEM((N_KV, ROPE_DIM, HALF_N), bf),
            pltpu.VMEM((W_SLOTS, W_ROWS, HALF_N), bf),
            pltpu.VMEM((KV_LAT, G_HEADS * 256), bf),
            pltpu.VMEM((RING, RING, RING, 2, ROWS, KV_W), bf),
            pltpu.VMEM((2, RING, 2, ROWS, Q_LAT), bf),
            pltpu.VMEM((2, RING, 2, ROWS, 128), f32),
            pltpu.VMEM((2, RING, G_HEADS, UNIT, Q_W), bf),
            pltpu.VMEM((2, RING, 2, ROWS, K_COLS), bf),
            pltpu.VMEM((GROUP, 2, 2, ROWS, K_COLS), bf),
            pltpu.VMEM((OUT_ROWS, HALF_N), f32),
            pltpu.VMEM((2, ROWS, HALF_N), bf),
            dma((2,)), dma((W_SLOTS,)), dma((N_KV,)), dma,
            dma((3, 3, 3)), dma((3, 3, 3)), dma((3, 2)), dma((3, 2)), dma((3, 4)), dma((3, 4)),
            dma((3,)), dma((3,)), dma((3,)), dma((3,)), dma((2, 4)), dma((2, 4)),
            dma((2, 3)), dma((2, 3)), dma((2, 4)), dma((2, 4)), dma((2,)), dma((2,)),
        ],
        compiler_params=pltpu.CompilerParams(collective_id=0, has_side_effects=True, vmem_limit_bytes=67043328),
        name="latent_attention_block",
    )(pos_one, pos_two, gain_q, gain_kv, x_one, x_two, w_qdown, w_kvdown, w_qup, w_kvup, w_out)
    y_shape = jax.ShapeDtypeStruct((ROWS, D_MODEL), bf)
    return pl.pallas_call(copy_kernel, out_shape=(y_shape, y_shape), in_specs=[vmem], out_specs=(vmem, vmem), name="results")(y)


def solution(mesh):
    tok_spec = P(('dp', 'sp'), None)
    idx_spec = P(('dp', 'sp'))

    def local_body(x_one, seg_one, pos_one, x_two, seg_two, pos_two, w_qdown, gain_q, w_qup, w_kvdown, gain_kv, w_kvup, w_out):
        return block(pos_one, pos_two, gain_q, gain_kv, x_one, x_two, w_qdown, w_kvdown.T, w_qup, w_kvup, w_out)

    return jax.shard_map(local_body, mesh=mesh, in_specs=(tok_spec, idx_spec, idx_spec, tok_spec, idx_spec, idx_spec, P(), P(), P(), P(), P(), P(), P()), out_specs=(tok_spec, tok_spec), check_vma=False)
```

```python
import jax
import jax.numpy as jnp
from jax import lax
from jax.experimental import pallas as pl
from jax.experimental.pallas import tpu as pltpu
from jax.sharding import PartitionSpec as P

D_MODEL = 7168
HEADS = 128
Q_LAT = 1536
KV_LAT = 512
ROPE_DIM = 64
NOPE_DIM = 128
V_DIM = 128
QK_DIM = NOPE_DIM + ROPE_DIM
KV_DOWN = KV_LAT + ROPE_DIM
ROPE_BASE = 10000.0
NORM_EPS = 1e-6

ROWS = 16
RING = 4
GROUP = 2 * RING
G_HEADS = HEADS // GROUP
TOKENS = 2048
KV_W = 2 * KV_LAT + 2 * ROPE_DIM
Q_W = KV_LAT + 2 * ROPE_DIM
UNIT = 2 * ROWS
G_ROWS = 2 * RING * UNIT
HALF_N = D_MODEL // 2
OUT_N = D_MODEL // 4
OUT_ROWS = 4 * UNIT
K_COLS = G_HEADS * V_DIM
MESH = pl.DeviceIdType.MESH

COLORS = (((0, 256), (2, 1, 0)), ((256, 640), (1, 0, 2)), ((640, 1152), (0, 2, 1)))

W_ROWS = 512
W_SLOTS = 8
N_KV = 2
N_DOWN = D_MODEL // W_ROWS
N_UP = Q_LAT // W_ROWS
N_OUT = HEADS * V_DIM // (2 * W_ROWS)
FIRST_UP = N_KV + N_DOWN
FIRST_OUT = FIRST_UP + N_UP
N_CHUNKS = FIRST_OUT + N_OUT
PER_RANK = K_COLS // (2 * W_ROWS)

ORDER = ((0, 0), (0, 1), (1, 0), (3, 0), (1, 1), (3, 1), (2, 0), (2, 1))


def coords():
    me = lax.axis_index("sp")
    return me // 32, lax.rem(me // 8, 4), lax.rem(me // 2, 4), lax.rem(me, 2)


def device(z, y, x, c):
    return {"sp": ((z * RING + y) * RING + x) * 2 + c}


def shifted(pos, axis, k):
    out = list(pos)
    out[axis] = lax.rem(pos[axis] + k, RING)
    return tuple(out)


def block_kernel(pos_one, pos_two, gain_q, gain_kv, x_one, x_two, wqd, wkvd, wqu, wkvu, wout, y_ref,
                 xs, qd, kd, kr_buf, w_buf, wkv, kv_ref, q_ref, tab_ref, q_eff, o_ref, o_all, acc, y_send,
                 x_sem, w_sem, w_sem2, kr_sem, wkv_sem, kv_send, kv_recv, r_send, r_recv, d_send, d_recv,
                 q_send, q_recv, t_send, t_recv, dq_send, dq_recv, a_send, a_recv, p_send, p_recv, y_ssem, y_rsem):
    z, y, x, c = coords()
    pos = (z, y, x)
    rank = z * 2 + c
    other = device(z, y, x, 1 - c)
    pair, member = z // 2, lax.rem(z, 2)
    mate = 2 * pair + 1 - member
    trans = (((1,), (1,)), ((), ()))

    def rank_at(j):
        out = jnp.int32(0)
        for i, (k, flip) in enumerate(ORDER):
            cc = c if flip == 0 else 1 - c
            out = jnp.where(j == i, lax.rem(z + RING - k, RING) * 2 + cc, out)
        return out

    def x_copy(i):
        return pltpu.make_async_copy((x_one, x_two)[i], xs.at[pl.ds(i * ROWS, ROWS), :], x_sem.at[i])

    def lat_copy(s):
        return pltpu.make_async_copy(wkvd.at[pl.ds(0, KV_LAT), pl.ds(s * HALF_N, HALF_N)], w_buf.at[s], w_sem.at[s])

    def kr_copy(s):
        return pltpu.make_async_copy(
            wkvd.at[pl.ds(KV_LAT, ROPE_DIM), pl.ds(s * HALF_N, HALF_N)], kr_buf.at[s], kr_sem.at[s])

    def down_copy(s):
        slot = lax.rem(s, W_SLOTS)
        return pltpu.make_async_copy(
            wqd.at[pl.ds(pl.multiple_of((s - N_KV) * W_ROWS, W_ROWS), W_ROWS), :], w_buf.at[slot, :, pl.ds(0, Q_LAT)], w_sem.at[slot])

    def up_copy(s):
        slot = lax.rem(s, W_SLOTS)
        width = G_HEADS * QK_DIM
        return pltpu.make_async_copy(
            wqu.at[pl.ds(pl.multiple_of((s - FIRST_UP) * W_ROWS, W_ROWS), W_ROWS), pl.ds(pl.multiple_of(rank * width, 128), width)],
            w_buf.at[slot, :, pl.ds(0, width)], w_sem.at[slot])

    def out_copies(s):
        slot = lax.rem(s, W_SLOTS)
        t = s - FIRST_OUT
        row = rank_at(t // PER_RANK) * K_COLS + lax.rem(t, PER_RANK) * (2 * W_ROWS)
        cols = pl.ds(pl.multiple_of((member * 2 + c) * OUT_N, 128), OUT_N)
        return [pltpu.make_async_copy(
            wout.at[pl.ds(pl.multiple_of(row + h * W_ROWS, W_ROWS), W_ROWS), cols],
            w_buf.at[slot, :, pl.ds(h * OUT_N, OUT_N)], sem.at[slot]) for h, sem in enumerate((w_sem, w_sem2))]

    def out_start(s):
        for copy in out_copies(s):
            copy.start()

    wkv_copy = pltpu.make_async_copy(
        wkvu.at[:, pl.ds(pl.multiple_of(rank * (G_HEADS * 256), 128), G_HEADS * 256)], wkv, wkv_sem)

    for i in range(2):
        x_copy(i).start()
    for s in range(N_KV):
        lat_copy(s).start()
        kr_copy(s).start()
    down_copy(jnp.int32(N_KV)).start()

    barrier = pltpu.get_barrier_semaphore()
    for axis in range(3):
        for k in range(1, RING):
            pl.semaphore_signal(barrier, inc=1, device_id=device(*shifted(pos, axis, k), c), device_id_type=MESH)
    pl.semaphore_signal(barrier, inc=1, device_id=other, device_id_type=MESH)
    pl.semaphore_signal(barrier, inc=1, device_id=device(mate, y, x, 1 - c), device_id_type=MESH)

    row16 = lax.broadcasted_iota(jnp.int32, (ROWS, 128), 0)
    lane16 = lax.broadcasted_iota(jnp.int32, (ROWS, 128), 1)
    freq = jnp.zeros((ROWS, 128), jnp.float32)
    for i in range(ROPE_DIM // 2):
        freq = jnp.where(lax.rem(lane16, ROPE_DIM // 2) == i, ROPE_BASE ** (-i / (ROPE_DIM // 2)), freq)
    tabs = []
    for mb, p_ref in enumerate((pos_one, pos_two)):
        at = jnp.zeros((ROWS, 128), jnp.float32)
        for i in range(ROWS):
            at = jnp.where(row16 == i, p_ref[i].astype(jnp.float32), at)
        angle = at * freq
        tabs.append(jnp.where(lane16 < 32, jnp.cos(angle), jnp.where(lane16 < 64, jnp.sin(angle), at)))
        tab_ref[mb, z, c] = tabs[mb]
    t0, t1 = tabs
    cos2 = jnp.where(lane16 < 32, t0, jnp.where(lane16 < 64, pltpu.roll(t0, 32, 1), jnp.where(lane16 < 96, pltpu.roll(t1, 64, 1), pltpu.roll(t1, 96, 1))))
    sin_hi = jnp.where((lane16 >= 32) & (lane16 < 64), t0, jnp.where(lane16 >= 96, pltpu.roll(t1, 64, 1), 0.0))
    sin_lo = jnp.where(lane16 < 32, -pltpu.roll(t0, 96, 1), jnp.where((lane16 >= 64) & (lane16 < 96), -pltpu.roll(t1, 32, 1), 0.0))

    kd[...] = jnp.zeros_like(kd)
    for i in range(2):
        x_copy(i).wait()
    for s in range(N_KV):
        rhs = xs[:, s * HALF_N:(s + 1) * HALF_N]
        lat_copy(s).wait()
        if s == 0:
            for i in range(N_KV + 1, W_SLOTS):
                down_copy(jnp.int32(i)).start()
        kd[:KV_LAT, :2 * ROWS] += lax.dot_general(w_buf[s], rhs, trans, preferred_element_type=jnp.float32)
        kr_copy(s).wait()
        kd[KV_LAT:KV_DOWN, :2 * ROWS] += lax.dot_general(kr_buf[s], rhs, trans, preferred_element_type=jnp.float32)
        down_copy(jnp.int32(s + W_SLOTS)).start()
    raw = jnp.transpose(kd[...])[:2 * ROWS]
    u = raw[:, :KV_LAT]
    lat = (u * lax.rsqrt(jnp.mean(u * u, axis=-1, keepdims=True) + NORM_EPS) * gain_kv[...].astype(jnp.float32)[None]).astype(jnp.bfloat16)
    kv_ref[z, y, x, c, :, 0:KV_LAT] = lat[:ROWS]
    kv_ref[z, y, x, c, :, KV_LAT:2 * KV_LAT] = lat[ROWS:]
    rot = jnp.where(lane16 < 64, raw[:ROWS, KV_LAT:], pltpu.roll(raw[ROWS:, KV_LAT:], 64, 1))
    rot = rot * cos2 + pltpu.roll(rot, 32, 1) * sin_hi + pltpu.roll(rot, 96, 1) * sin_lo
    kv_ref[z, y, x, c, :, 2 * KV_LAT:] = rot.astype(jnp.bfloat16)
    qd[...] = jnp.zeros_like(qd)
    pl.semaphore_wait(barrier, 11)

    def q_down(lo, hi):
        @pl.loop(lo, hi)
        def _(i):
            s = i + N_KV
            lhs = xs[:, pl.ds(pl.multiple_of(i * W_ROWS, W_ROWS), W_ROWS)]
            down_copy(s).wait()
            qd[...] += jnp.dot(lhs, w_buf[lax.rem(s, W_SLOTS), :, :Q_LAT], preferred_element_type=jnp.float32)

            @pl.when(s + W_SLOTS < FIRST_UP)
            def _():
                down_copy(s + W_SLOTS).start()

    def kv_piece(color, phase, at, core, half=None):
        (lo, hi), order = COLORS[color]
        index = [at[0], at[1], at[2]]
        for axis in order[:phase]:
            index[axis] = slice(None)
        if half is not None:
            index[order[0]] = pl.ds(2 * half, 2)
        return kv_ref.at[index[0], index[1], index[2], core, :, pl.ds(lo, hi - lo)]

    def remote(piece, send, recv, to):
        return pltpu.make_async_remote_copy(
            src_ref=piece, dst_ref=piece, send_sem=send, recv_sem=recv, device_id=to, device_id_type=MESH)

    def kv_copy(color, phase, k, at, to):
        return remote(kv_piece(color, phase, at, c), kv_send.at[color, phase, k - 1], kv_recv.at[color, phase, k - 1], to)

    def relay_copy(color, half, at, to):
        return remote(kv_piece(color, 2, at, c, half), r_send.at[color, half], r_recv.at[color, half], to)

    def pass_copy(color, k, at, core):
        return remote(kv_piece(color, 2, at, core), d_send.at[color, k], d_recv.at[color, k], other)

    def q_copy(zz, cc, to, send, recv):
        return remote(q_ref.at[:, zz, cc], send, recv, to)

    def t_copy(zz, cc, to, send, recv):
        return remote(tab_ref.at[:, zz, cc], send, recv, to)

    def start_phase(phase):
        for color in range(3):
            axis = COLORS[color][1][phase]
            for k in (1, 3, 2) if phase < 2 else (1, 3):
                kv_copy(color, phase, k, pos, device(*shifted(pos, axis, k), c)).start()

    def wait_phase(phase):
        for k in (1, 3, 2):
            for color in range(3):
                kv_copy(color, phase, k, shifted(pos, COLORS[color][1][phase], RING - k), other).wait_recv()

    start_phase(0)
    q_down(0, N_DOWN // 2)
    wait_phase(0)
    start_phase(1)
    q_down(N_DOWN // 2, N_DOWN)
    for s in range(FIRST_UP, FIRST_UP + W_SLOTS):
        if s < FIRST_OUT:
            up_copy(jnp.int32(s)).start()
        if s == FIRST_OUT:
            wkv_copy.start()
        if s >= FIRST_OUT:
            out_start(jnp.int32(s))
    v = qd[...]
    q_lat = (v * lax.rsqrt(jnp.mean(v * v, axis=-1, keepdims=True) + NORM_EPS) * gain_q[...].astype(jnp.float32)[None]).astype(jnp.bfloat16)
    q_ref[:, z, c] = q_lat.reshape(2, ROWS, Q_LAT)
    for k in (2, 1, 3):
        to = device(*shifted(pos, 0, k), c)
        t_copy(z, c, to, t_send.at[k - 1], t_recv.at[k - 1]).start()
        q_copy(z, c, to, q_send.at[k - 1], q_recv.at[k - 1]).start()
    t_copy(z, c, other, dq_send.at[0, 0], dq_recv.at[0, 0]).start()
    q_copy(z, c, other, dq_send.at[1, 0], dq_recv.at[1, 0]).start()
    wait_phase(1)
    start_phase(2)
    for color in range(3):
        pass_copy(color, 0, pos, c).start()
    for k in (1, 3, 2):
        zz = lax.rem(z + RING - k, RING)
        t_copy(zz, c, other, t_send.at[k - 1], t_recv.at[k - 1]).wait_recv()
        t_copy(zz, c, other, dq_send.at[0, k], dq_recv.at[0, k]).start()
        q_copy(zz, c, other, q_send.at[k - 1], q_recv.at[k - 1]).wait_recv()
        q_copy(zz, c, other, dq_send.at[1, k], dq_recv.at[1, k]).start()

    for k in (1, 3):
        for color in (1, 2, 0):
            axis = COLORS[color][1][2]
            source = shifted(pos, axis, RING - k)
            kv_copy(color, 2, k, source, other).wait_recv()
            relay_copy(color, k // 2, source, device(*shifted(pos, axis, k), c)).start()
            pass_copy(color, k, source, c).start()
    for k in range(RING):
        zz = lax.rem(z + RING - k, RING)
        t_copy(zz, 1 - c, other, dq_send.at[0, k], dq_recv.at[0, k]).wait()
        q_copy(zz, 1 - c, other, dq_send.at[1, k], dq_recv.at[1, k]).wait()

    q2 = q_ref.reshape(G_ROWS, Q_LAT)
    tab2 = tab_ref.reshape(G_ROWS, 128)
    kv2 = kv_ref.reshape(TOKENS, KV_W)
    lane = lax.broadcasted_iota(jnp.int32, (G_ROWS, 128), 1)
    tab = tab2[...]
    cos_t = jnp.where(lane < 32, tab, jnp.where(lane < 64, pltpu.roll(tab, 32, 1), 0.0))
    sin_b = jnp.where((lane >= 32) & (lane < 64), tab, 0.0)
    sin_a = jnp.where(lane < 32, -pltpu.roll(tab, 96, 1), 0.0)

    def put_rope(head, part):
        out = part * cos_t + pltpu.roll(part, 32, 1) * sin_b + pltpu.roll(part, 96, 1) * sin_a
        half = G_ROWS // 2
        out = jnp.concatenate([out[:half], pltpu.roll(out[half:], 64, 1)], axis=0)
        q_eff[:, :, head, :, KV_LAT:] = out.astype(jnp.bfloat16).reshape(2, RING, UNIT, 128)

    def put_nope(head, part):
        w_k = wkv[:, pl.ds(pl.multiple_of(head * 256, 256), 128)]
        out = lax.dot_general(part.astype(jnp.bfloat16), w_k, (((1,), (1,)), ((), ())), preferred_element_type=jnp.float32)
        q_eff[:, :, head, :, :KV_LAT] = out.astype(jnp.bfloat16).reshape(2, RING, UNIT, KV_LAT)

    for s in range(FIRST_UP, FIRST_OUT):
        up_copy(jnp.int32(s)).wait()
    wkv_copy.wait()

    def queries(lo, hi):
        @pl.loop(lo, hi)
        def _(g):
            parts = []
            for i in range(2):
                cols = pl.ds(pl.multiple_of((2 * g + i) * (2 * QK_DIM), 128), 2 * QK_DIM)
                f = jnp.zeros((G_ROWS, 2 * QK_DIM), jnp.float32)
                for n in range(N_UP):
                    f = f + jnp.dot(q2[:, n * W_ROWS:(n + 1) * W_ROWS], w_buf[(FIRST_UP + n) % W_SLOTS, :, cols],
                                    preferred_element_type=jnp.float32)
                parts.append(f)
            for i, f in enumerate(parts):
                head = 4 * g + 2 * i
                put_nope(head, f[:, :128])
                put_rope(head, f[:, 128:256])
                mid = pltpu.roll(f[:, 128:256], 64, 1)
                last = pltpu.roll(f[:, 256:384], 64, 1)
                put_nope(head + 1, jnp.where(lane < 64, mid, last))
                put_rope(head + 1, last)

    queries(0, G_HEADS // 4)
    for s in range(FIRST_UP + W_SLOTS, FIRST_OUT + W_SLOTS):
        out_start(jnp.int32(s))

    for color in range(3):
        source = shifted(pos, COLORS[color][1][2], 2)
        for half in range(2):
            relay_copy(color, half, source, other).wait_recv()
        pass_copy(color, 2, source, c).start()
    for k in (0, 1, 3, 2):
        for color in range(3):
            pass_copy(color, k, shifted(pos, COLORS[color][1][2], RING - k), 1 - c).wait_recv()

    def ring_copy(mb, k, zz, src_rank, to):
        return pltpu.make_async_remote_copy(
            src_ref=o_ref.at[mb, pl.ds(2 * (zz // 2), 2)], dst_ref=o_all.at[src_rank, mb], send_sem=a_send.at[mb, k - 1],
            recv_sem=a_recv.at[mb, k - 1], device_id=to, device_id_type=MESH)

    def pair_copy(mb, k, src_rank, src):
        return pltpu.make_async_remote_copy(
            src_ref=src, dst_ref=o_all.at[src_rank, mb], send_sem=p_send.at[mb, k], recv_sem=p_recv.at[mb, k],
            device_id=other, device_id_type=MESH)

    scale2 = (QK_DIM ** -0.5) * 1.4426950408889634
    tok = lax.broadcasted_iota(jnp.int32, (UNIT, 1), 0)

    @pl.loop(0, 2)
    def _(mb):
        lat_cols = pl.ds(pl.multiple_of(mb * KV_LAT, KV_LAT), KV_LAT)
        for zz in range(RING):
            length = (zz + 1) * 512
            key = lax.broadcasted_iota(jnp.int32, (UNIT, length), 1)
            q_tok = zz * 512 + y * 128 + x * 32 + tok
            p0 = tab2[pl.ds(pl.multiple_of((mb * RING + zz) * UNIT, UNIT), UNIT), 64:65].astype(jnp.int32)
            cap = jnp.where((key <= q_tok) & (key >= q_tok - p0), 3e38, -1e30).astype(jnp.float32)
            q = q_eff[mb, zz].reshape(G_HEADS * UNIT, Q_W)
            keys = kv2[:length, lat_cols]
            s = lax.dot_general(q[:, :KV_LAT], keys, trans, preferred_element_type=jnp.float32)
            s = s + lax.dot_general(q[:, KV_LAT:], kv2[:length, 2 * KV_LAT:], trans, preferred_element_type=jnp.float32)
            s = jnp.minimum(s.reshape(G_HEADS, UNIT, length), cap[None])
            top = jnp.max(s, axis=-1, keepdims=True)
            e = jnp.exp2((s - top) * scale2)
            total = jnp.sum(e, axis=-1, keepdims=True)
            e = e.astype(jnp.bfloat16).reshape(G_HEADS * UNIT, length)
            o = jnp.dot(e, keys, preferred_element_type=jnp.float32).reshape(G_HEADS, UNIT, KV_LAT)
            q_eff[mb, zz, :, :, :KV_LAT] = (o / total).astype(jnp.bfloat16)

        @pl.loop(0, G_HEADS // 4)
        def _(g):
            for i in range(4):
                h = g * 4 + i
                w_v = wkv[:, pl.ds(pl.multiple_of(h * 256 + 128, 128), 128)]
                o_h = jnp.dot(q_eff[mb, :, h, :, :KV_LAT].reshape(RING * UNIT, KV_LAT), w_v, preferred_element_type=jnp.float32)
                o_ref[mb, :, :, :, pl.ds(pl.multiple_of(h * 128, 128), 128)] = o_h.astype(jnp.bfloat16).reshape(RING, 2, ROWS, V_DIM)

        for k in (1, 3, 2):
            zz = lax.rem(z + k, RING)
            ring_copy(mb, k, zz, rank, device(zz, y, x, c)).start()
        pair_copy(mb, 0, rank, o_ref.at[mb, pl.ds(2 * pair, 2)]).start()

    o_all[rank] = o_ref[:, pl.ds(2 * pair, 2)]
    acc[...] = jnp.zeros_like(acc)

    def arrive(mb, k):
        src_rank = lax.rem(z + RING - k, RING) * 2 + c
        ring_copy(mb, k, z, src_rank, other).wait_recv()
        pair_copy(mb, k, src_rank, o_all.at[src_rank, mb]).start()

    arrive(0, 1)
    arrive(0, 3)

    @pl.loop(0, N_OUT)
    def _(t):
        for i, (k, flip) in enumerate(ORDER):
            if i == 0:
                continue

            @pl.when(t == i * PER_RANK)
            def _(k=k, flip=flip):
                if flip == 0:
                    if k == 2:
                        arrive(0, k)
                    arrive(1, k)
                else:
                    src_rank = lax.rem(z + RING - k, RING) * 2 + 1 - c
                    for mb in range(2):
                        pair_copy(mb, k, src_rank, o_all.at[src_rank, mb]).wait_recv()

        s = t + FIRST_OUT
        src = rank_at(t // PER_RANK)
        k0 = lax.rem(t, PER_RANK) * (2 * W_ROWS)
        lhs = [o_all[src, :, :, :, :, pl.ds(pl.multiple_of(k0 + h * W_ROWS, W_ROWS), W_ROWS)].reshape(OUT_ROWS, W_ROWS) for h in range(2)]
        for copy in out_copies(s):
            copy.wait()
        slot = lax.rem(s, W_SLOTS)
        for lo in range(0, OUT_N, 512):
            hi = min(lo + 512, OUT_N)
            acc[:, lo:hi] += (jnp.dot(lhs[0], w_buf[slot, :, lo:hi], preferred_element_type=jnp.float32)
                              + jnp.dot(lhs[1], w_buf[slot, :, OUT_N + lo:OUT_N + hi], preferred_element_type=jnp.float32))

        @pl.when(s + W_SLOTS < N_CHUNKS)
        def _():
            out_start(s + W_SLOTS)

    acc5 = acc.reshape(2, 2, 2, ROWS, OUT_N)
    owners = ((member, 1 - c), (1 - member, c), (1 - member, 1 - c))

    def col_part(mm, cc):
        return pl.ds(pl.multiple_of((mm * 2 + cc) * OUT_N, 128), OUT_N)

    def y_copy(d, cols):
        mm, cc = owners[d]
        return pltpu.make_async_remote_copy(
            src_ref=y_send.at[d], dst_ref=y_ref.at[:, :, cols], send_sem=y_ssem.at[d], recv_sem=y_rsem.at[d],
            device_id=device(2 * pair + mm, y, x, cc), device_id_type=MESH)

    for d in (2, 1, 0):
        for mb in range(2):
            y_send[d, mb] = acc5[mb, owners[d][0], owners[d][1]].astype(jnp.bfloat16)
    for mb in range(2):
        y_ref[mb, :, col_part(member, c)] = acc5[mb, member, c].astype(jnp.bfloat16)
    for d in (2, 1, 0):
        y_copy(d, col_part(member, c)).start()

    for k in range(1, RING):
        t_copy(z, c, other, t_send.at[k - 1], t_recv.at[k - 1]).wait_send()
        q_copy(z, c, other, q_send.at[k - 1], q_recv.at[k - 1]).wait_send()
        for color in range(3):
            for phase in range(3):
                if phase < 2 or k != 2:
                    kv_copy(color, phase, k, pos, other).wait_send()
    for color in range(3):
        for half in range(2):
            relay_copy(color, half, pos, other).wait_send()
        for k in range(RING):
            pass_copy(color, k, pos, c).wait_send()
    for mb in range(2):
        for k in range(1, RING):
            ring_copy(mb, k, z, rank, other).wait_send()
        for k in range(RING):
            pair_copy(mb, k, rank, o_all.at[rank, mb]).wait_send()
    for d in range(3):
        y_copy(d, col_part(*owners[d])).wait()


def copy_kernel(y_ref, y_one, y_two):
    y_one[...] = y_ref[0]
    y_two[...] = y_ref[1]


def block(pos_one, pos_two, gain_q, gain_kv, x_one, x_two, w_qdown, w_kvdown, w_qup, w_kvup, w_out):
    dma = pltpu.SemaphoreType.DMA
    vmem = pl.BlockSpec(memory_space=pltpu.VMEM)
    smem = pl.BlockSpec(memory_space=pltpu.SMEM)
    hbm = pl.BlockSpec(memory_space=pl.ANY)
    bf, f32 = jnp.bfloat16, jnp.float32
    y = pl.pallas_call(
        block_kernel,
        out_shape=jax.ShapeDtypeStruct((2, ROWS, D_MODEL), bf),
        in_specs=[smem] * 2 + [vmem] * 2 + [hbm] * 7,
        out_specs=vmem,
        scratch_shapes=[
            pltpu.VMEM((2 * ROWS, D_MODEL), bf),
            pltpu.VMEM((2 * ROWS, Q_LAT), f32),
            pltpu.VMEM((KV_LAT + 128, 128), f32),
            pltpu.VMEM((N_KV, ROPE_DIM, HALF_N), bf),
            pltpu.VMEM((W_SLOTS, W_ROWS, HALF_N), bf),
            pltpu.VMEM((KV_LAT, G_HEADS * 256), bf),
            pltpu.VMEM((RING, RING, RING, 2, ROWS, KV_W), bf),
            pltpu.VMEM((2, RING, 2, ROWS, Q_LAT), bf),
            pltpu.VMEM((2, RING, 2, ROWS, 128), f32),
            pltpu.VMEM((2, RING, G_HEADS, UNIT, Q_W), bf),
            pltpu.VMEM((2, RING, 2, ROWS, K_COLS), bf),
            pltpu.VMEM((GROUP, 2, 2, 2, ROWS, K_COLS), bf),
            pltpu.VMEM((OUT_ROWS, OUT_N), f32),
            pltpu.VMEM((3, 2, ROWS, OUT_N), bf),
            dma((2,)), dma((W_SLOTS,)), dma((W_SLOTS,)), dma((N_KV,)), dma,
            dma((3, 3, 3)), dma((3, 3, 3)), dma((3, 2)), dma((3, 2)), dma((3, 4)), dma((3, 4)),
            dma((3,)), dma((3,)), dma((3,)), dma((3,)), dma((2, 4)), dma((2, 4)),
            dma((2, 3)), dma((2, 3)), dma((2, 4)), dma((2, 4)), dma((3,)), dma((3,)),
        ],
        compiler_params=pltpu.CompilerParams(collective_id=0, has_side_effects=True, vmem_limit_bytes=67043328),
        name="latent_attention_block",
    )(pos_one, pos_two, gain_q, gain_kv, x_one, x_two, w_qdown, w_kvdown, w_qup, w_kvup, w_out)
    y_shape = jax.ShapeDtypeStruct((ROWS, D_MODEL), bf)
    return pl.pallas_call(copy_kernel, out_shape=(y_shape, y_shape), in_specs=[vmem], out_specs=(vmem, vmem), name="results")(y)


def solution(mesh):
    tok_spec = P(('dp', 'sp'), None)
    idx_spec = P(('dp', 'sp'))

    def local_body(x_one, seg_one, pos_one, x_two, seg_two, pos_two, w_qdown, gain_q, w_qup, w_kvdown, gain_kv, w_kvup, w_out):
        return block(pos_one, pos_two, gain_q, gain_kv, x_one, x_two, w_qdown, w_kvdown.T, w_qup, w_kvup, w_out)

    return jax.shard_map(local_body, mesh=mesh, in_specs=(tok_spec, idx_spec, idx_spec, tok_spec, idx_spec, idx_spec, P(), P(), P(), P(), P(), P(), P()), out_specs=(tok_spec, tok_spec), check_vma=False)
```
